32 devices in a mesh: clips: 1, frame: 32 (over z, y, x, core).
Axes of the slice: x: 2, y: 2, z: 4, core: 2. Of those that a mesh axis runs over, the one named last changes fastest.
Arguments:
- frame_sequence_elements: bfloat16 [32, 256, 1280], P(('clips', 'frame')), may hold values from -8 to 8
- entry_rescaling_factors: float32 [1280], replicated, may hold values from 0.5 to 1.5
- asking_projection_tensor: bfloat16 [1280, 640], replicated, may hold values from -1 to 1
- lookup_projection_tensor: bfloat16 [1280, 640], replicated, may hold values from -1 to 1
- content_projection_tensor: bfloat16 [1280, 640], replicated, may hold values from -0.15625 to 0.15625
- logit_sharpness: float32 [5], replicated, may hold values from 0.3 to 24
- final_projection_tensor: bfloat16 [640, 1280], replicated, may hold values from -0.25 to 0.25
Outputs:
- mixed: bfloat16 [32, 256, 1280], P(('clips', 'frame'))
The draws below stay inside these ranges and needn't reach their ends.
All inputs are finite; a program needn't handle non-finite values.
Results may differ from the reference program's by a relative error of at most 0.006.
Values may be sent and summed in bfloat16 or wider, within the bound.
A program may use at most 64 MiB of HBM per device.

```python
import math
import jax
import jax.numpy as jnp
from jax import lax

D = 1280
HEADS_WIN = 5
CHANNELS_PER_ATT = 128
S = 256
WINDOW = 32
QW = 640
FRAMES = 32


def draw_frame_sequence_elements(key, part):
    values = jax.random.normal(jax.random.fold_in(key, 1), (FRAMES, S, D), jnp.float32)
    return jnp.clip(values, -8.0, 8.0).astype(jnp.bfloat16)


def shared_rows(key):
    return jnp.clip(jax.random.normal(jax.random.fold_in(key, 7), (D, QW), jnp.float32), -6.0, 6.0)


def draw_asking_projection_tensor(key, part):
    return (shared_rows(key) / math.sqrt(D)).astype(jnp.bfloat16)


def draw_lookup_projection_tensor(key, part):
    jitter = jnp.clip(jax.random.normal(jax.random.fold_in(key, 13), (D, QW), jnp.float32), -6.0, 6.0)
    values = jitter / math.sqrt(D)
    return values.astype(jnp.bfloat16)


def draw_logit_sharpness(key, part):
    lower, upper = (0.3, 3.0)
    level = jax.random.uniform(jax.random.fold_in(key, 17), (HEADS_WIN,), jnp.float32, math.log(lower), math.log(upper))
    return jnp.exp(level)


def centred(own_key, extent, width, reach, kind=jnp.bfloat16):
    return jnp.clip(width * jax.random.normal(own_key, extent, jnp.float32), -reach, reach).astype(kind)


def setup_inputs(seed: int = 0, part: int = 0) -> dict:
    splits = jax.random.split(jax.random.key(seed), 8)
    part_keys = jax.random.split(jax.random.fold_in(splits[7], part), 8)
    frame_sequence_elements = draw_frame_sequence_elements(jax.random.fold_in(jax.random.fold_in(splits[7], part), 71), part)
    entry_rescaling_factors = jnp.clip(1.0 + 0.1 * jax.random.normal(splits[1], (D,), jnp.float32), 0.5, 1.5)
    asking_projection_tensor = draw_asking_projection_tensor(jax.random.fold_in(splits[7], 71), part)
    lookup_projection_tensor = draw_lookup_projection_tensor(jax.random.fold_in(splits[7], 71), part)
    content_projection_tensor = centred(splits[4], (D, QW), D ** -0.5, 0.15625)
    logit_sharpness = draw_logit_sharpness(jax.random.fold_in(splits[7], 71), part)
    final_projection_tensor = centred(splits[6], (QW, D), QW ** -0.5, 0.25)
    return dict(frame_sequence_elements=frame_sequence_elements, entry_rescaling_factors=entry_rescaling_factors, asking_projection_tensor=asking_projection_tensor, lookup_projection_tensor=lookup_projection_tensor, content_projection_tensor=content_projection_tensor, logit_sharpness=logit_sharpness, final_projection_tensor=final_projection_tensor)


epsilon = 1e-06

def quadratic_average_rescaling(values):
    return values * lax.rsqrt(lax.optimization_barrier(jnp.mean(values * values, axis=-1, keepdims=True)) + epsilon)

def reference(frame_sequence_elements, entry_rescaling_factors, asking_projection_tensor, lookup_projection_tensor, content_projection_tensor, logit_sharpness, final_projection_tensor):
    floated = frame_sequence_elements.astype(jnp.float32)
    rescaled_token_vectors = (quadratic_average_rescaling(floated) * entry_rescaling_factors).astype(jnp.bfloat16)
    flat_rows = rescaled_token_vectors.reshape(FRAMES * S, D)
    shape_heads = (FRAMES, S, HEADS_WIN, CHANNELS_PER_ATT)
    asking_vectors_full = jnp.dot(flat_rows, asking_projection_tensor, preferred_element_type=jnp.float32).reshape(shape_heads)
    k_full = jnp.dot(flat_rows, lookup_projection_tensor, preferred_element_type=jnp.float32).reshape(shape_heads)
    v_full = jnp.dot(flat_rows, content_projection_tensor, preferred_element_type=jnp.float32).reshape(shape_heads)
    asking_token_vectors = (quadratic_average_rescaling(asking_vectors_full) * logit_sharpness[:, None] / math.sqrt(CHANNELS_PER_ATT)).astype(jnp.bfloat16)
    key_matrix_rows = quadratic_average_rescaling(k_full).astype(jnp.bfloat16)
    value_matrix_rows = v_full.astype(jnp.bfloat16)
    frame_ids = jnp.arange(FRAMES, dtype=jnp.int32)
    offset = frame_ids[:, None] - frame_ids[None, :]
    window_mask = (offset >= 0) & (offset < WINDOW)

    def column(pieces):
        q_col, k_col, v_col = pieces
        scores = jnp.einsum('thd,shd->hts', q_col.astype(jnp.float32), k_col.astype(jnp.float32))
        scores = jnp.where(window_mask[None], scores, -1e+30)
        top = lax.optimization_barrier(jnp.max(scores, axis=-1, keepdims=True))
        expo = jnp.exp(scores - top)
        weights = (expo / lax.optimization_barrier(jnp.sum(expo, axis=-1, keepdims=True))).astype(jnp.bfloat16)
        attended = jnp.einsum('hts,shd->thd', weights.astype(jnp.float32), v_col.astype(jnp.float32))
        return attended.astype(jnp.bfloat16)
    per_column = lax.map(column, (asking_token_vectors.transpose(1, 0, 2, 3), key_matrix_rows.transpose(1, 0, 2, 3), value_matrix_rows.transpose(1, 0, 2, 3)))
    attended = per_column.transpose(1, 0, 2, 3).reshape(FRAMES * S, QW)
    summed = jnp.dot(attended, final_projection_tensor, preferred_element_type=jnp.float32) + floated.reshape(FRAMES * S, D)
    return summed.astype(jnp.bfloat16).reshape(FRAMES, S, D)
```

```python
import functools
import math

import jax
import jax.numpy as jnp
from jax import lax
from jax.experimental import pallas as pl
from jax.experimental.pallas import tpu as pltpu
from jax.sharding import PartitionSpec as P

HEADS_WIN = 5
CHANNELS_PER_ATT = 128
WINDOW = 32


epsilon = 1e-06


def quadratic_average_rescaling(values):
    return values * lax.rsqrt(jnp.mean(values * values, axis=-1, keepdims=True) + epsilon)


def project_through(
    incoming_token_vectors,
    asking_projection_tensor,
    lookup_projection_tensor,
    content_projection_tensor,
    logit_sharpness,
):
    lead = incoming_token_vectors.shape[:-1]
    flat_rows = incoming_token_vectors.reshape(-1, incoming_token_vectors.shape[-1])
    shape_heads = lead + (HEADS_WIN, CHANNELS_PER_ATT)
    asking_vectors_full = jnp.dot(
        flat_rows, asking_projection_tensor, preferred_element_type=jnp.float32
    ).reshape(shape_heads)
    k_full = jnp.dot(
        flat_rows, lookup_projection_tensor, preferred_element_type=jnp.float32
    ).reshape(shape_heads)
    v_full = jnp.dot(
        flat_rows, content_projection_tensor, preferred_element_type=jnp.float32
    ).reshape(shape_heads)
    asking_token_vectors = (
        quadratic_average_rescaling(asking_vectors_full)
        * logit_sharpness[:, None]
        / math.sqrt(CHANNELS_PER_ATT)
    ).astype(jnp.bfloat16)
    key_matrix_rows = quadratic_average_rescaling(k_full).astype(jnp.bfloat16)
    return (asking_token_vectors, key_matrix_rows, v_full.astype(jnp.bfloat16))


def softmax_bf16(scores, window_mask):
    scores = jnp.where(window_mask, scores, -1e30)
    top = jnp.max(scores, axis=-1, keepdims=True)
    expo = jnp.exp(scores - top)
    return (expo / jnp.sum(expo, axis=-1, keepdims=True)).astype(jnp.bfloat16)


def band_attention(asking_token_vectors, key_matrix_rows, value_matrix_rows):
    all_frames, positions, heads, width = asking_token_vectors.shape
    blocks = all_frames // WINDOW
    block_shape = (blocks, WINDOW, positions, heads, width)
    q_blocks = asking_token_vectors.reshape(block_shape)
    k_blocks = key_matrix_rows.reshape(block_shape)
    v_blocks = value_matrix_rows.reshape(block_shape)
    k_earlier = jnp.concatenate([jnp.zeros_like(k_blocks[:1]), k_blocks[:-1]], axis=0)
    v_earlier = jnp.concatenate([jnp.zeros_like(v_blocks[:1]), v_blocks[:-1]], axis=0)
    k_pair = jnp.concatenate([k_earlier, k_blocks], axis=1)
    v_pair = jnp.concatenate([v_earlier, v_blocks], axis=1)
    scores = jnp.einsum("bqphd,bkphd->bphqk", q_blocks, k_pair, preferred_element_type=jnp.float32)
    block_ids = jnp.arange(blocks, dtype=jnp.int32)[:, None, None]
    row_ids = jnp.arange(WINDOW, dtype=jnp.int32)[None, :, None]
    col_ids = jnp.arange(2 * WINDOW, dtype=jnp.int32)[None, None, :]
    offset = row_ids - col_ids + WINDOW
    inside = (offset >= 0) & (offset < WINDOW) & (block_ids * WINDOW - WINDOW + col_ids >= 0)
    weights = softmax_bf16(scores, inside[:, None, None])
    attended = jnp.einsum("bphqk,bkphd->bqphd", weights, v_pair, preferred_element_type=jnp.float32)
    return attended.astype(jnp.bfloat16).reshape(all_frames, positions, heads, width)


def local(
    frame_sequence_elements,
    entry_rescaling_factors,
    asking_projection_tensor,
    lookup_projection_tensor,
    content_projection_tensor,
    logit_sharpness,
    final_projection_tensor,
):
    frames_dev, seq_len, width = frame_sequence_elements.shape
    floated = frame_sequence_elements.astype(jnp.float32)
    rescaled_token_vectors = (
        quadratic_average_rescaling(floated) * entry_rescaling_factors
    ).astype(jnp.bfloat16)
    position_rows = lax.all_to_all(
        rescaled_token_vectors, "frame", split_axis=1, concat_axis=0, tiled=True
    )
    asking_token_vectors, key_matrix_rows, value_matrix_rows = project_through(
        position_rows,
        asking_projection_tensor,
        lookup_projection_tensor,
        content_projection_tensor,
        logit_sharpness,
    )
    result = band_attention(asking_token_vectors, key_matrix_rows, value_matrix_rows)
    attended = lax.all_to_all(result, "frame", split_axis=0, concat_axis=1, tiled=True)
    flat_attended = attended.reshape(frames_dev * seq_len, -1)
    summed = jnp.dot(
        flat_attended, final_projection_tensor, preferred_element_type=jnp.float32
    ) + floated.reshape(frames_dev * seq_len, width)
    return summed.astype(jnp.bfloat16).reshape(frames_dev, seq_len, width)


MESH = pl.DeviceIdType.MESH
HIGH = HEADS_WIN * CHANNELS_PER_ATT


def fused(
    devices,
    local_frames,
    sharp_ref,
    x_hbm,
    gain_ref,
    wq_hbm,
    wk_hbm,
    wv_hbm,
    wo_hbm,
    out_ref,
    x_own,
    wq,
    wk,
    wv,
    wo,
    gathered,
    q_rows,
    k_rows,
    v_rows,
    outgoing,
    returned,
    load_sem,
    ready,
    send_a,
    recv_a,
    send_b,
    recv_b,
):
    me = lax.axis_index("frame")
    block, width = x_own.shape[1], x_own.shape[2]
    positions = block // local_frames
    chips = devices // 2
    depth = chips // 4
    chip, side = me // 2, lax.rem(me, 2)
    partner = me + 1 - 2 * side
    z, y, x = chip // 4, lax.rem(chip // 2, 2), lax.rem(chip, 2)

    def other(dz, dy, dx):
        tz = lax.rem(z + dz, depth)
        ty = y + dy - 2 * dy * y
        tx = x + dx - 2 * dx * x
        above = (tz >= z) & (ty >= y) & (tx >= x)
        below = (tz <= z) & (ty <= y) & (tx <= x)
        return tz * 4 + ty * 2 + tx, above, below

    steps = [(dz, dy, dx) for dz in range(depth) for dy in range(2) for dx in range(2)][1:]
    far_first = sorted(steps, key=lambda s: (s[0] == 0, s[0]))
    near_first = sorted(steps, key=lambda s: (sum(s), s[0]))

    barrier = pltpu.get_barrier_semaphore()

    def signal(semaphore, target):
        pl.semaphore_signal(
            semaphore, inc=1, device_id={"frame": target}, device_id_type=MESH
        )

    signal(barrier, partner)
    for step in near_first:
        there, above, _ = other(*step)

        @pl.when(above)
        def _():
            signal(barrier, there * 2)
            signal(barrier, there * 2 + 1)

    loads = [
        pltpu.make_async_copy(source, target, load_sem.at[i])
        for i, (source, target) in enumerate(
            ((x_hbm, x_own), (wq_hbm, wq), (wk_hbm, wk), (wv_hbm, wv), (wo_hbm, wo))
        )
    ]
    for load in loads:
        load.start()
    pl.semaphore_wait(barrier, 2 * ((z + 1) * (y + 1) * (x + 1) - 1) + 1)
    for step in far_first:
        there, _, below = other(*step)

        @pl.when(below)
        def _():
            signal(ready.at[chip], there * 2)
            signal(ready.at[chip], there * 2 + 1)

    loads[0].wait()

    def send_tokens(target):
        pltpu.make_async_remote_copy(
            src_ref=x_own.at[target],
            dst_ref=gathered.at[me],
            send_sem=send_a,
            recv_sem=recv_a.at[z // 2],
            device_id={"frame": target},
            device_id_type=MESH,
        ).start()

    send_tokens(partner)
    for step in far_first:
        there, _, below = other(*step)

        @pl.when(below)
        def _():
            send_tokens(there * 2)

    for step in near_first:
        there, above, _ = other(*step)

        @pl.when(above)
        def _():
            pl.semaphore_wait(ready.at[there], 2)
            send_tokens(there * 2)

    for step in near_first:
        there, above, below = other(*step)

        @pl.when(jnp.logical_not(above | below))
        def _():
            send_tokens(there * 2)

    for step in far_first:
        there, _, _ = other(*step)
        send_tokens(there * 2 + 1)
    gathered[me] = x_own[me]
    for load in loads[1:]:
        load.wait()

    half = devices // 2
    rows = half * block

    def arrived(ref, semaphore):
        pltpu.make_async_remote_copy(
            src_ref=ref,
            dst_ref=ref,
            send_sem=send_a,
            recv_sem=semaphore,
            device_id={"frame": partner},
            device_id_type=MESH,
        ).wait_recv()

    def departed(ref, semaphore):
        pltpu.make_async_remote_copy(
            src_ref=ref,
            dst_ref=ref,
            send_sem=semaphore,
            recv_sem=recv_a.at[0],
            device_id={"frame": partner},
            device_id_type=MESH,
        ).wait_send()

    def project(part):
        tokens = gathered[pl.ds(part * half, half)].astype(jnp.float32).reshape(rows, width)
        normed = (quadratic_average_rescaling(tokens) * gain_ref[...].reshape(1, width)).astype(
            jnp.bfloat16
        )
        q = jnp.dot(normed, wq[...], preferred_element_type=jnp.float32)
        k = jnp.dot(normed, wk[...], preferred_element_type=jnp.float32)
        v = jnp.dot(normed, wv[...], preferred_element_type=jnp.float32)
        to = pl.ds(pl.multiple_of(part * rows, rows), rows)
        for h in range(HEADS_WIN):
            c = slice(h * CHANNELS_PER_ATT, (h + 1) * CHANNELS_PER_ATT)
            q_rows[to, c] = (
                quadratic_average_rescaling(q[:, c]) * sharp_ref[h] / math.sqrt(CHANNELS_PER_ATT)
            ).astype(jnp.bfloat16)
            k_rows[to, c] = quadratic_average_rescaling(k[:, c]).astype(jnp.bfloat16)
            v_rows[to, c] = v[:, c].astype(jnp.bfloat16)

    mine = z // 2
    arrived(gathered.at[pl.ds(0, half - 1)], recv_a.at[mine])
    project(mine)
    arrived(gathered.at[pl.ds(0, half)], recv_a.at[1 - mine])
    project(1 - mine)

    total = devices * block

    def ids(axis):
        shape = (total, 1) if axis == 0 else (1, total)
        r = lax.broadcasted_iota(jnp.int32, shape, axis)
        owner = r // block
        inner = r - owner * block
        return owner * local_frames + inner // positions, inner % positions

    t_row, p_row = ids(0)
    t_col, p_col = ids(1)
    offset = t_row - t_col
    inside = (p_row == p_col) & (offset >= 0) & (offset < WINDOW)
    for h in range(HEADS_WIN):
        c = slice(h * CHANNELS_PER_ATT, (h + 1) * CHANNELS_PER_ATT)
        scores = lax.dot_general(
            q_rows[:, c], k_rows[:, c], (((1,), (1,)), ((), ())), preferred_element_type=jnp.float32
        )
        weights = softmax_bf16(scores, inside)
        attended = jnp.dot(weights, v_rows[:, c], preferred_element_type=jnp.float32)
        outgoing[:, :, c] = attended.reshape(devices, block, CHANNELS_PER_ATT).astype(jnp.bfloat16)

    def send_back(target):
        pltpu.make_async_remote_copy(
            src_ref=outgoing.at[target],
            dst_ref=returned.at[side, chip],
            send_sem=send_b,
            recv_sem=recv_b.at[side],
            device_id={"frame": target},
            device_id_type=MESH,
        ).start()

    for step in far_first:
        there, _, _ = other(*step)
        send_back(there * 2)
        send_back(there * 2 + 1)
    send_back(partner)
    returned[side, chip] = outgoing[me]

    def finish(s):
        mixed = returned[s].astype(jnp.float32).reshape(rows, HIGH).astype(jnp.bfloat16)
        summed = jnp.dot(mixed, wo[...], preferred_element_type=jnp.float32)
        for k in range(chips):
            j = 2 * k + s
            out_ref[j] = (
                summed[k * block : (k + 1) * block] + x_own[j].astype(jnp.float32)
            ).astype(jnp.bfloat16)

    for s in range(2):

        @pl.when(side == s)
        def _():
            arrived(returned.at[s, pl.ds(0, chips - 1)], recv_b.at[s])

        @pl.when(side != s)
        def _():
            arrived(returned.at[s], recv_b.at[s])

        finish(s)
    departed(x_own.at[pl.ds(0, devices - 1)], send_a)
    departed(outgoing.at[pl.ds(0, devices - 1)], send_b)


def local_fused(devices, x, gain, wq, wk, wv, sharp, wo):
    local_frames, seq_len, width = x.shape
    positions = seq_len // devices
    block = local_frames * positions
    total = devices * block
    blocks = x.reshape(local_frames, devices, positions, width)
    blocks = blocks.transpose(1, 0, 2, 3).reshape(devices, block, width)
    vmem = pl.BlockSpec(memory_space=pltpu.VMEM)
    anywhere = pl.BlockSpec(memory_space=pl.ANY)
    dma = pltpu.SemaphoreType.DMA
    out = pl.pallas_call(
        functools.partial(fused, devices, local_frames),
        out_shape=pltpu.VMEM(blocks.shape, jnp.bfloat16),
        in_specs=[pl.BlockSpec(memory_space=pltpu.SMEM), anywhere, vmem] + [anywhere] * 4,
        out_specs=vmem,
        scratch_shapes=[
            pltpu.VMEM(blocks.shape, jnp.bfloat16),
            pltpu.VMEM(wq.shape, jnp.bfloat16),
            pltpu.VMEM(wk.shape, jnp.bfloat16),
            pltpu.VMEM(wv.shape, jnp.bfloat16),
            pltpu.VMEM(wo.shape, jnp.bfloat16),
            pltpu.VMEM(blocks.shape, jnp.bfloat16),
            pltpu.VMEM((total, HIGH), jnp.bfloat16),
            pltpu.VMEM((total, HIGH), jnp.bfloat16),
            pltpu.VMEM((total, HIGH), jnp.bfloat16),
            pltpu.VMEM((devices, block, HIGH), jnp.bfloat16),
            pltpu.VMEM((2, devices // 2, block, HIGH), jnp.bfloat16),
            dma((5,)),
            pltpu.SemaphoreType.REGULAR((devices // 2,)),
            dma,
            dma((2,)),
            dma,
            dma((2,)),
        ],
        compiler_params=pltpu.CompilerParams(
            collective_id=0, has_side_effects=True, vmem_limit_bytes=60 * 2**20
        ),
    )(sharp, blocks, gain, wq, wk, wv, wo)
    out = out.reshape(devices, local_frames, positions, width).transpose(1, 0, 2, 3)
    return out.reshape(x.shape)


def solution(mesh):
    devices = mesh.shape["frame"]

    def body(x, *rest):
        positions = x.shape[1] // devices
        if devices % 16 == 0 and positions % 8 == 0:
            return local_fused(devices, x, *rest)
        return local(x, *rest)

    placed = (P(("clips", "frame"), None, None), P(), P(), P(), P(), P(), P())
    return jax.shard_map(
        body,
        mesh=mesh,
        in_specs=placed,
        out_specs=P(("clips", "frame"), None, None),
        check_vma=False,
    )
```

```python
import functools
import math

import jax
import jax.numpy as jnp
from jax import lax
from jax.experimental import pallas as pl
from jax.experimental.pallas import tpu as pltpu
from jax.sharding import PartitionSpec as P

HEADS_WIN = 5
CHANNELS_PER_ATT = 128
WINDOW = 32


epsilon = 1e-06


def quadratic_average_rescaling(values):
    return values * lax.rsqrt(jnp.mean(values * values, axis=-1, keepdims=True) + epsilon)


def project_through(
    incoming_token_vectors,
    asking_projection_tensor,
    lookup_projection_tensor,
    content_projection_tensor,
    logit_sharpness,
):
    lead = incoming_token_vectors.shape[:-1]
    flat_rows = incoming_token_vectors.reshape(-1, incoming_token_vectors.shape[-1])
    shape_heads = lead + (HEADS_WIN, CHANNELS_PER_ATT)
    asking_vectors_full = jnp.dot(
        flat_rows, asking_projection_tensor, preferred_element_type=jnp.float32
    ).reshape(shape_heads)
    k_full = jnp.dot(
        flat_rows, lookup_projection_tensor, preferred_element_type=jnp.float32
    ).reshape(shape_heads)
    v_full = jnp.dot(
        flat_rows, content_projection_tensor, preferred_element_type=jnp.float32
    ).reshape(shape_heads)
    asking_token_vectors = (
        quadratic_average_rescaling(asking_vectors_full)
        * logit_sharpness[:, None]
        / math.sqrt(CHANNELS_PER_ATT)
    ).astype(jnp.bfloat16)
    key_matrix_rows = quadratic_average_rescaling(k_full).astype(jnp.bfloat16)
    return (asking_token_vectors, key_matrix_rows, v_full.astype(jnp.bfloat16))


def softmax_bf16(scores, window_mask):
    scores = jnp.where(window_mask, scores, -1e30)
    top = jnp.max(scores, axis=-1, keepdims=True)
    expo = jnp.exp(scores - top)
    return (expo / jnp.sum(expo, axis=-1, keepdims=True)).astype(jnp.bfloat16)


def band_attention(asking_token_vectors, key_matrix_rows, value_matrix_rows):
    all_frames, positions, heads, width = asking_token_vectors.shape
    blocks = all_frames // WINDOW
    block_shape = (blocks, WINDOW, positions, heads, width)
    q_blocks = asking_token_vectors.reshape(block_shape)
    k_blocks = key_matrix_rows.reshape(block_shape)
    v_blocks = value_matrix_rows.reshape(block_shape)
    k_earlier = jnp.concatenate([jnp.zeros_like(k_blocks[:1]), k_blocks[:-1]], axis=0)
    v_earlier = jnp.concatenate([jnp.zeros_like(v_blocks[:1]), v_blocks[:-1]], axis=0)
    k_pair = jnp.concatenate([k_earlier, k_blocks], axis=1)
    v_pair = jnp.concatenate([v_earlier, v_blocks], axis=1)
    scores = jnp.einsum("bqphd,bkphd->bphqk", q_blocks, k_pair, preferred_element_type=jnp.float32)
    block_ids = jnp.arange(blocks, dtype=jnp.int32)[:, None, None]
    row_ids = jnp.arange(WINDOW, dtype=jnp.int32)[None, :, None]
    col_ids = jnp.arange(2 * WINDOW, dtype=jnp.int32)[None, None, :]
    offset = row_ids - col_ids + WINDOW
    inside = (offset >= 0) & (offset < WINDOW) & (block_ids * WINDOW - WINDOW + col_ids >= 0)
    weights = softmax_bf16(scores, inside[:, None, None])
    attended = jnp.einsum("bphqk,bkphd->bqphd", weights, v_pair, preferred_element_type=jnp.float32)
    return attended.astype(jnp.bfloat16).reshape(all_frames, positions, heads, width)


def local(
    frame_sequence_elements,
    entry_rescaling_factors,
    asking_projection_tensor,
    lookup_projection_tensor,
    content_projection_tensor,
    logit_sharpness,
    final_projection_tensor,
):
    frames_dev, seq_len, width = frame_sequence_elements.shape
    floated = frame_sequence_elements.astype(jnp.float32)
    rescaled_token_vectors = (
        quadratic_average_rescaling(floated) * entry_rescaling_factors
    ).astype(jnp.bfloat16)
    position_rows = lax.all_to_all(
        rescaled_token_vectors, "frame", split_axis=1, concat_axis=0, tiled=True
    )
    asking_token_vectors, key_matrix_rows, value_matrix_rows = project_through(
        position_rows,
        asking_projection_tensor,
        lookup_projection_tensor,
        content_projection_tensor,
        logit_sharpness,
    )
    result = band_attention(asking_token_vectors, key_matrix_rows, value_matrix_rows)
    attended = lax.all_to_all(result, "frame", split_axis=0, concat_axis=1, tiled=True)
    flat_attended = attended.reshape(frames_dev * seq_len, -1)
    summed = jnp.dot(
        flat_attended, final_projection_tensor, preferred_element_type=jnp.float32
    ) + floated.reshape(frames_dev * seq_len, width)
    return summed.astype(jnp.bfloat16).reshape(frames_dev, seq_len, width)


MESH = pl.DeviceIdType.MESH
HIGH = HEADS_WIN * CHANNELS_PER_ATT


def fused(
    devices,
    local_frames,
    sharp_hbm,
    x_hbm,
    gain_hbm,
    wq_hbm,
    wk_hbm,
    wv_hbm,
    wo_hbm,
    out_ref,
    sharp_ref,
    gain_ref,
    x_own,
    wq,
    wk,
    wv,
    wo,
    gathered,
    extra,
    q_rows,
    k_rows,
    v_rows,
    outgoing,
    outgoing_extra,
    returned,
    load_sem,
    ready,
    send_a,
    send_x,
    recv_a,
    recv_x,
    send_b,
    send_c,
    recv_b,
):
    me = lax.axis_index("frame")
    block, width = x_own.shape[1], x_own.shape[2]
    positions = block // local_frames
    chips = devices // 2
    depth = chips // 4
    half = devices // 2
    rows = half * block
    chip, side = me // 2, lax.rem(me, 2)
    partner = me + 1 - 2 * side
    z, y, x = chip // 4, lax.rem(chip // 2, 2), lax.rem(chip, 2)
    low = me < half

    def other(dz, dy, dx):
        tz = lax.rem(z + dz, depth)
        ty = y + dy - 2 * dy * y
        tx = x + dx - 2 * dx * x
        above = (tz >= z) & (ty >= y) & (tx >= x)
        below = (tz <= z) & (ty <= y) & (tx <= x)
        return tz * 4 + ty * 2 + tx, above, below

    steps = [(dz, dy, dx) for dz in range(depth) for dy in range(2) for dx in range(2)][1:]
    far_first = sorted(steps, key=lambda s: (s[0] == 0, s[0]))
    near_first = sorted(steps, key=lambda s: (sum(s), s[0]))

    x_load = pltpu.make_async_copy(x_hbm, x_own, load_sem.at[0])
    x_load.start()
    barrier = pltpu.get_barrier_semaphore()

    def signal(semaphore, target):
        pl.semaphore_signal(
            semaphore, inc=1, device_id={"frame": target}, device_id_type=MESH
        )

    signal(barrier, partner)
    for step in near_first:
        there, above, _ = other(*step)

        @pl.when(above)
        def _():
            signal(barrier, there * 2)
            signal(barrier, there * 2 + 1)

    loads = [
        pltpu.make_async_copy(source, target, load_sem.at[i + 1])
        for i, (source, target) in enumerate(
            (
                (sharp_hbm, sharp_ref),
                (gain_hbm, gain_ref),
                (wq_hbm, wq),
                (wk_hbm, wk),
                (wv_hbm, wv),
                (wo_hbm, wo),
            )
        )
    ]
    for load in loads:
        load.start()
    with jax.named_scope("barrier"):
        pl.semaphore_wait(barrier, 2 * ((z + 1) * (y + 1) * (x + 1) - 1) + 1)
    for step in far_first:
        there, _, below = other(*step)

        @pl.when(below)
        def _():
            signal(ready.at[chip], there * 2)
            signal(ready.at[chip], there * 2 + 1)

    with jax.named_scope("load_x"):
        x_load.wait()

    def remote(source, target, send, recv, device):
        pltpu.make_async_remote_copy(
            src_ref=source,
            dst_ref=target,
            send_sem=send,
            recv_sem=recv,
            device_id={"frame": device},
            device_id_type=MESH,
        ).start()

    group = me // half

    def send_tokens(target):
        remote(x_own.at[target], gathered.at[me], send_a, recv_a.at[group], target)

    def send_extra(target):
        remote(x_own.at[target + half], extra.at[me], send_x, recv_x, target)

    with jax.named_scope("send_below"):
        send_tokens(partner)
        for step in far_first:
            there, _, below = other(*step)

            @pl.when(below)
            def _():
                send_tokens(there * 2)

    with jax.named_scope("send_above"):
        for step in near_first:
            there, above, _ = other(*step)

            @pl.when(above)
            def _():
                pl.semaphore_wait(ready.at[there], 2)
                send_tokens(there * 2)

    with jax.named_scope("send_rest"):
        for step in near_first:
            there, above, below = other(*step)

            @pl.when(jnp.logical_not(above | below))
            def _():
                send_tokens(there * 2)

        def send_late(level):
            for there in reversed(range(chips)):
                if there // 2 % 2 == level:

                    @pl.when(there != chip)
                    def _():
                        send_tokens(there * 2 + 1)

        def send_extras(to):
            @pl.when(low)
            def _():
                for there in reversed(range(half // 2)):
                    @pl.when(there * 2 + to != me)
                    def _():
                        send_extra(there * 2 + to)

        send_late(0)
        send_extras(1)
        send_late(1)
        send_extras(0)

        @pl.when(low)
        def _():
            extra[me] = x_own[me + half]

        gathered[me] = x_own[me]
        for load in loads:
            load.wait()

    def arrived(ref, semaphore):
        pltpu.make_async_remote_copy(
            src_ref=ref,
            dst_ref=ref,
            send_sem=send_a,
            recv_sem=semaphore,
            device_id={"frame": partner},
            device_id_type=MESH,
        ).wait_recv()

    def departed(ref, semaphore):
        pltpu.make_async_remote_copy(
            src_ref=ref,
            dst_ref=ref,
            send_sem=semaphore,
            recv_sem=recv_x,
            device_id={"frame": partner},
            device_id_type=MESH,
        ).wait_send()

    def project(tokens, places, ask=True):
        tokens = tokens.astype(jnp.float32)
        normed = (quadratic_average_rescaling(tokens) * gain_ref[...].reshape(1, width)).astype(
            jnp.bfloat16
        )
        q = jnp.dot(normed, wq[...], preferred_element_type=jnp.float32) if ask else None
        k = jnp.dot(normed, wk[...], preferred_element_type=jnp.float32)
        v = jnp.dot(normed, wv[...], preferred_element_type=jnp.float32)
        for h in range(HEADS_WIN):
            c = slice(h * CHANNELS_PER_ATT, (h + 1) * CHANNELS_PER_ATT)
            ks = quadratic_average_rescaling(k[:, c]).astype(jnp.bfloat16)
            vs = v[:, c].astype(jnp.bfloat16)
            if ask:
                qs = (
                    quadratic_average_rescaling(q[:, c]) * sharp_ref[h] / math.sqrt(CHANNELS_PER_ATT)
                ).astype(jnp.bfloat16)
            for i, place in enumerate(places):
                a = slice(i * rows, (i + 1) * rows)
                b = slice(place * rows, (place + 1) * rows)
                k_rows[b, c] = ks[a]
                v_rows[b, c] = vs[a]
                if ask:
                    q_rows[b, c] = qs[a]

    def ids(first, count, axis):
        shape = (count, 1) if axis == 0 else (1, count)
        r = first + lax.broadcasted_iota(jnp.int32, shape, axis)
        owner = r // block
        inner = r - owner * block
        return owner * local_frames + inner // positions, inner % positions

    def attend(asking, keys, target):
        first, count = asking
        start, length = keys
        base = 2 * rows if start >= 2 * rows else 0
        t_row, p_row = ids(first - base, count, 0)
        t_col, p_col = ids(start - base, length, 1)
        offset = t_row - t_col
        inside = (p_row == p_col) & (offset >= 0) & (offset < WINDOW)
        a, b = slice(first, first + count), slice(start, start + length)
        heads = [slice(h * CHANNELS_PER_ATT, (h + 1) * CHANNELS_PER_ATT) for h in range(HEADS_WIN)]
        scores = [
            lax.dot_general(
                q_rows[a, c],
                k_rows[b, c],
                (((1,), (1,)), ((), ())),
                preferred_element_type=jnp.float32,
            )
            for c in heads
        ]
        weights = [softmax_bf16(s, inside) for s in scores]
        attended = [
            jnp.dot(w, v_rows[b, c], preferred_element_type=jnp.float32)
            for w, c in zip(weights, heads)
        ]
        for c, part in zip(heads, attended):
            target[:, :, c] = part.reshape(half, block, CHANNELS_PER_ATT).astype(jnp.bfloat16)

    def tokens_of(part):
        return gathered[part * half : (part + 1) * half].reshape(rows, width)

    def send_back(target):
        remote(outgoing.at[target], returned.at[me], send_b, recv_b.at[group], target)

    def back_to_high():
        for k in range(half // 2):
            there = half // 2 + lax.rem(chip + k, half // 2)
            for s in range(2):
                target = there * 2 + s

                @pl.when(target != me)
                def _():
                    send_back(target)

    @pl.when(low)
    def _():
        with jax.named_scope("wait_own"):
            arrived(gathered.at[pl.ds(0, half - 1)], recv_a.at[0])
        with jax.named_scope("work_own"):
            project(tokens_of(0), (0,))
            attend((0, rows), (0, rows), outgoing.at[pl.ds(0, half)])
            for k in range(1, half):
                send_back(lax.rem(me + k, half))
            returned[me] = outgoing[me]
        def extras():
            with jax.named_scope("wait_extra"):
                arrived(extra.at[pl.ds(0, half - 1)], recv_x)
            with jax.named_scope("work_extra"):
                project(extra[...].reshape(rows, width), (2,))
                attend((2 * rows, rows), (2 * rows, rows), outgoing_extra)
                for k in range(1, half):
                    target = lax.rem(me + k, half)
                    remote(
                        outgoing_extra.at[target],
                        returned.at[me + half],
                        send_c,
                        recv_b.at[1],
                        target,
                    )
                returned[me + half] = outgoing_extra[me]

        pl.when(side == 1)(extras)
        with jax.named_scope("wait_far"):
            arrived(gathered.at[pl.ds(0, half)], recv_a.at[1])
        with jax.named_scope("work_far"):
            project(tokens_of(1), (1,))
            attend((rows, rows), (0, 2 * rows), outgoing.at[pl.ds(half, half)])
            back_to_high()
        pl.when(side == 0)(extras)

    @pl.when(jnp.logical_not(low))
    def _():
        with jax.named_scope("wait_own"):
            arrived(gathered.at[pl.ds(0, half - 1)], recv_a.at[1])
        with jax.named_scope("work_own"):
            project(tokens_of(1), (1,))
        with jax.named_scope("wait_far"):
            arrived(gathered.at[pl.ds(0, half)], recv_a.at[0])
        with jax.named_scope("work_far"):
            project(tokens_of(0), (0,), ask=False)
            attend((rows, rows), (0, 2 * rows), outgoing.at[pl.ds(half, half)])
            back_to_high()
            returned[me] = outgoing[me]

    def finish(part):
        span = slice(part * half, (part + 1) * half)
        mixed = returned[span].reshape(rows, HIGH)
        summed = jnp.dot(mixed, wo[...], preferred_element_type=jnp.float32)
        for k in range(half):
            j = part * half + k
            out_ref[j] = (
                summed[k * block : (k + 1) * block] + x_own[j].astype(jnp.float32)
            ).astype(jnp.bfloat16)

    @pl.when(low)
    def _():
        with jax.named_scope("wait_b0"):
            arrived(returned.at[pl.ds(0, half - 1)], recv_b.at[0])
        with jax.named_scope("finish0"):
            finish(0)
        with jax.named_scope("wait_b1"):
            arrived(returned.at[pl.ds(0, half - 1)], recv_b.at[1])
        with jax.named_scope("finish1"):
            finish(1)

    @pl.when(jnp.logical_not(low))
    def _():
        with jax.named_scope("wait_b1"):
            arrived(returned.at[pl.ds(0, half - 1)], recv_b.at[1])
        with jax.named_scope("finish1"):
            finish(1)
        with jax.named_scope("wait_b0"):
            arrived(returned.at[pl.ds(0, half)], recv_b.at[0])
        with jax.named_scope("finish0"):
            finish(0)

    with jax.named_scope("departed"):
        departed(x_own.at[pl.ds(0, devices - 1)], send_a)

        @pl.when(low)
        def _():
            departed(x_own.at[pl.ds(0, half - 1)], send_x)
            departed(outgoing.at[pl.ds(0, devices - 1)], send_b)
            departed(outgoing_extra.at[pl.ds(0, half - 1)], send_c)

        @pl.when(jnp.logical_not(low))
        def _():
            departed(outgoing.at[pl.ds(0, half - 1)], send_b)


def local_fused(devices, x, gain, wq, wk, wv, sharp, wo):
    local_frames, seq_len, width = x.shape
    positions = seq_len // devices
    block = local_frames * positions
    half = devices // 2
    rows = half * block
    blocks = x.reshape(local_frames, devices, positions, width)
    blocks = blocks.transpose(1, 0, 2, 3).reshape(devices, block, width)
    vmem = pl.BlockSpec(memory_space=pltpu.VMEM)
    anywhere = pl.BlockSpec(memory_space=pl.ANY)
    dma = pltpu.SemaphoreType.DMA
    out = pl.pallas_call(
        functools.partial(fused, devices, local_frames),
        out_shape=pltpu.VMEM(blocks.shape, jnp.bfloat16),
        in_specs=[anywhere] * 7,
        out_specs=vmem,
        scratch_shapes=[
            pltpu.SMEM(sharp.shape, jnp.float32),
            pltpu.VMEM(gain.shape, jnp.float32),
            pltpu.VMEM(blocks.shape, jnp.bfloat16),
            pltpu.VMEM(wq.shape, jnp.bfloat16),
            pltpu.VMEM(wk.shape, jnp.bfloat16),
            pltpu.VMEM(wv.shape, jnp.bfloat16),
            pltpu.VMEM(wo.shape, jnp.bfloat16),
            pltpu.VMEM(blocks.shape, jnp.bfloat16),
            pltpu.VMEM((half, block, width), jnp.bfloat16),
            pltpu.VMEM((3 * rows, HIGH), jnp.bfloat16),
            pltpu.VMEM((3 * rows, HIGH), jnp.bfloat16),
            pltpu.VMEM((3 * rows, HIGH), jnp.bfloat16),
            pltpu.VMEM((devices, block, HIGH), jnp.bfloat16),
            pltpu.VMEM((half, block, HIGH), jnp.bfloat16),
            pltpu.VMEM((devices, block, HIGH), jnp.bfloat16),
            dma((7,)),
            pltpu.SemaphoreType.REGULAR((devices // 2,)),
            dma,
            dma,
            dma((2,)),
            dma,
            dma,
            dma,
            dma((2,)),
        ],
        compiler_params=pltpu.CompilerParams(
            collective_id=0, has_side_effects=True, vmem_limit_bytes=60 * 2**20
        ),
    )(sharp, blocks, gain, wq, wk, wv, wo)
    out = out.reshape(devices, local_frames, positions, width).transpose(1, 0, 2, 3)
    return out.reshape(x.shape)


def solution(mesh):
    devices = mesh.shape["frame"]

    def body(x, *rest):
        positions = x.shape[1] // devices
        if devices % 16 == 0 and positions % 8 == 0:
            return local_fused(devices, x, *rest)
        return local(x, *rest)

    placed = (P(("clips", "frame"), None, None), P(), P(), P(), P(), P(), P())
    return jax.shard_map(
        body,
        mesh=mesh,
        in_specs=placed,
        out_specs=P(("clips", "frame"), None, None),
        check_vma=False,
    )
```

```python
import functools
import math

import jax
import jax.numpy as jnp
from jax import lax
from jax.experimental import pallas as pl
from jax.experimental.pallas import tpu as pltpu
from jax.sharding import PartitionSpec as P

HEADS_WIN = 5
CHANNELS_PER_ATT = 128
WINDOW = 32


epsilon = 1e-06


def quadratic_average_rescaling(values):
    return values * lax.rsqrt(jnp.mean(values * values, axis=-1, keepdims=True) + epsilon)


def project_through(
    incoming_token_vectors,
    asking_projection_tensor,
    lookup_projection_tensor,
    content_projection_tensor,
    logit_sharpness,
):
    lead = incoming_token_vectors.shape[:-1]
    flat_rows = incoming_token_vectors.reshape(-1, incoming_token_vectors.shape[-1])
    shape_heads = lead + (HEADS_WIN, CHANNELS_PER_ATT)
    asking_vectors_full = jnp.dot(
        flat_rows, asking_projection_tensor, preferred_element_type=jnp.float32
    ).reshape(shape_heads)
    k_full = jnp.dot(
        flat_rows, lookup_projection_tensor, preferred_element_type=jnp.float32
    ).reshape(shape_heads)
    v_full = jnp.dot(
        flat_rows, content_projection_tensor, preferred_element_type=jnp.float32
    ).reshape(shape_heads)
    asking_token_vectors = (
        quadratic_average_rescaling(asking_vectors_full)
        * logit_sharpness[:, None]
        / math.sqrt(CHANNELS_PER_ATT)
    ).astype(jnp.bfloat16)
    key_matrix_rows = quadratic_average_rescaling(k_full).astype(jnp.bfloat16)
    return (asking_token_vectors, key_matrix_rows, v_full.astype(jnp.bfloat16))


def softmax_bf16(scores, window_mask):
    scores = jnp.where(window_mask, scores, -1e30)
    top = jnp.max(scores, axis=-1, keepdims=True)
    expo = jnp.exp(scores - top)
    return (expo / jnp.sum(expo, axis=-1, keepdims=True)).astype(jnp.bfloat16)


def band_attention(asking_token_vectors, key_matrix_rows, value_matrix_rows):
    all_frames, positions, heads, width = asking_token_vectors.shape
    blocks = all_frames // WINDOW
    block_shape = (blocks, WINDOW, positions, heads, width)
    q_blocks = asking_token_vectors.reshape(block_shape)
    k_blocks = key_matrix_rows.reshape(block_shape)
    v_blocks = value_matrix_rows.reshape(block_shape)
    k_earlier = jnp.concatenate([jnp.zeros_like(k_blocks[:1]), k_blocks[:-1]], axis=0)
    v_earlier = jnp.concatenate([jnp.zeros_like(v_blocks[:1]), v_blocks[:-1]], axis=0)
    k_pair = jnp.concatenate([k_earlier, k_blocks], axis=1)
    v_pair = jnp.concatenate([v_earlier, v_blocks], axis=1)
    scores = jnp.einsum("bqphd,bkphd->bphqk", q_blocks, k_pair, preferred_element_type=jnp.float32)
    block_ids = jnp.arange(blocks, dtype=jnp.int32)[:, None, None]
    row_ids = jnp.arange(WINDOW, dtype=jnp.int32)[None, :, None]
    col_ids = jnp.arange(2 * WINDOW, dtype=jnp.int32)[None, None, :]
    offset = row_ids - col_ids + WINDOW
    inside = (offset >= 0) & (offset < WINDOW) & (block_ids * WINDOW - WINDOW + col_ids >= 0)
    weights = softmax_bf16(scores, inside[:, None, None])
    attended = jnp.einsum("bphqk,bkphd->bqphd", weights, v_pair, preferred_element_type=jnp.float32)
    return attended.astype(jnp.bfloat16).reshape(all_frames, positions, heads, width)


def local(
    frame_sequence_elements,
    entry_rescaling_factors,
    asking_projection_tensor,
    lookup_projection_tensor,
    content_projection_tensor,
    logit_sharpness,
    final_projection_tensor,
):
    frames_dev, seq_len, width = frame_sequence_elements.shape
    floated = frame_sequence_elements.astype(jnp.float32)
    rescaled_token_vectors = (
        quadratic_average_rescaling(floated) * entry_rescaling_factors
    ).astype(jnp.bfloat16)
    position_rows = lax.all_to_all(
        rescaled_token_vectors, "frame", split_axis=1, concat_axis=0, tiled=True
    )
    asking_token_vectors, key_matrix_rows, value_matrix_rows = project_through(
        position_rows,
        asking_projection_tensor,
        lookup_projection_tensor,
        content_projection_tensor,
        logit_sharpness,
    )
    result = band_attention(asking_token_vectors, key_matrix_rows, value_matrix_rows)
    attended = lax.all_to_all(result, "frame", split_axis=0, concat_axis=1, tiled=True)
    flat_attended = attended.reshape(frames_dev * seq_len, -1)
    summed = jnp.dot(
        flat_attended, final_projection_tensor, preferred_element_type=jnp.float32
    ) + floated.reshape(frames_dev * seq_len, width)
    return summed.astype(jnp.bfloat16).reshape(frames_dev, seq_len, width)


MESH = pl.DeviceIdType.MESH
HIGH = HEADS_WIN * CHANNELS_PER_ATT


def fused(
    devices,
    local_frames,
    sharp_hbm,
    x_hbm,
    gain_hbm,
    wq_hbm,
    wk_hbm,
    wv_hbm,
    wo_hbm,
    done_ref,
    left_ref,
    x_own,
    wo,
    sharp_ref,
    gain_ref,
    wq,
    wk,
    wv,
    gathered,
    extra,
    q_rows,
    k_rows,
    v_rows,
    outgoing,
    outgoing_extra,
    returned,
    load_sem,
    ready,
    send_a,
    send_x,
    recv_a,
    recv_x,
    send_b,
    send_c,
    recv_b,
):
    me = lax.axis_index("frame")
    block, width = x_own.shape[1], x_own.shape[2]
    positions = block // local_frames
    chips = devices // 2
    depth = chips // 4
    half = devices // 2
    rows = half * block
    chip, side = me // 2, lax.rem(me, 2)
    partner = me + 1 - 2 * side
    z, y, x = chip // 4, lax.rem(chip // 2, 2), lax.rem(chip, 2)
    low = me < half

    def other(dz, dy, dx):
        tz = lax.rem(z + dz, depth)
        ty = y + dy - 2 * dy * y
        tx = x + dx - 2 * dx * x
        above = (tz >= z) & (ty >= y) & (tx >= x)
        below = (tz <= z) & (ty <= y) & (tx <= x)
        return tz * 4 + ty * 2 + tx, above, below

    steps = [(dz, dy, dx) for dz in range(depth) for dy in range(2) for dx in range(2)][1:]
    far_first = sorted(steps, key=lambda s: (s[0] == 0, s[0]))
    near_first = sorted(steps, key=lambda s: (sum(s), s[0]))

    x_load = pltpu.make_async_copy(x_hbm, x_own, load_sem.at[0])
    x_load.start()
    barrier = pltpu.get_barrier_semaphore()

    def signal(semaphore, target):
        pl.semaphore_signal(
            semaphore, inc=1, device_id={"frame": target}, device_id_type=MESH
        )

    signal(barrier, partner)
    for step in near_first:
        there, above, _ = other(*step)

        @pl.when(above)
        def _():
            signal(barrier, there * 2)
            signal(barrier, there * 2 + 1)

    loads = [
        pltpu.make_async_copy(source, target, load_sem.at[i + 1])
        for i, (source, target) in enumerate(
            (
                (sharp_hbm, sharp_ref),
                (gain_hbm, gain_ref),
                (wq_hbm, wq),
                (wk_hbm, wk),
                (wv_hbm, wv),
                (wo_hbm, wo),
            )
        )
    ]
    for load in loads:
        load.start()
    with jax.named_scope("barrier"):
        pl.semaphore_wait(barrier, 2 * ((z + 1) * (y + 1) * (x + 1) - 1) + 1)
    for step in far_first:
        there, _, below = other(*step)

        @pl.when(below)
        def _():
            signal(ready.at[chip], there * 2)
            signal(ready.at[chip], there * 2 + 1)

    with jax.named_scope("load_x"):
        x_load.wait()

    def remote(source, target, send, recv, device):
        pltpu.make_async_remote_copy(
            src_ref=source,
            dst_ref=target,
            send_sem=send,
            recv_sem=recv,
            device_id={"frame": device},
            device_id_type=MESH,
        ).start()

    group = me // half

    def send_tokens(target):
        remote(x_own.at[target], gathered.at[me], send_a, recv_a.at[group], target)

    def send_extra(target):
        remote(x_own.at[target + 1 + half], extra.at[me], send_x, recv_x, target)

    shelf = depth // 2
    inner = z < shelf - 1

    def send_four(there):
        for s in range(2):
            send_tokens(there * 2 + s)
        send_extra(there * 2)

    with jax.named_scope("send_first"):
        send_tokens(partner)

        @pl.when(low & (side == 1))
        def _():
            send_extra(partner)

        @pl.when(low & (side == 0))
        def _():
            extra[me] = x_own[me + 1 + half]

        gathered[me] = x_own[me]

    def plane(step):
        return lax.rem(z + step[0], depth)

    def each_below(act):
        for step in far_first:
            there, _, below = other(*step)
            pl.when(below)(functools.partial(act, there))

    def each_joined(wanted, act):
        for step in near_first:
            dz, dy, dx = step
            there, above, _ = other(*step)

            @pl.when(above & wanted(step))
            def _():
                pl.semaphore_wait(ready.at[there], 2)
                act(there, step)
                ty, tx = lax.rem(there // 2, 2), lax.rem(there, 2)
                for p in range(depth) if dz == 0 else (None,):
                    tz = there // 4 if p is None else p
                    for ey in range(2 - dy):
                        for ex in range(2 - dx):
                            found = (y >= ey) & (x >= ex)
                            if p is not None:
                                found &= (p < z) | ((p == z) & (ey + ex > 0))
                            elif ey + ex == 0:
                                continue
                            pl.when(found)(
                                functools.partial(
                                    act, tz * 4 + (ty - ey) * 2 + tx - ex, step
                                )
                            )

    @pl.when(inner)
    def _():
        with jax.named_scope("send_group"):
            each_below(send_four)
            each_joined(lambda step: plane(step) < shelf, lambda there, step: send_four(there))

        with jax.named_scope("send_across"):
            each_joined(
                lambda step: plane(step) >= shelf, lambda there, step: send_tokens(there * 2)
            )
            for step in near_first:
                there, _, _ = other(*step)

                @pl.when(plane(step) >= shelf)
                def _():
                    send_tokens(there * 2 + 1)

    @pl.when(jnp.logical_not(inner))
    def _():
        with jax.named_scope("send_below"):
            each_below(lambda there: send_tokens(there * 2))

        with jax.named_scope("send_above"):
            each_joined(lambda step: True, lambda there, step: send_tokens(there * 2))

        with jax.named_scope("send_rest"):

            @pl.when(low)
            def _():
                for k in range(1, half // 2):
                    there = lax.rem(chip + k, half // 2)
                    send_tokens(there * 2 + 1)
                    send_extra(there * 2)

            for i in range(depth):
                tz = lax.rem((1 - group) * shelf + i, depth)
                for dy in range(2):
                    for dx in range(2):
                        there, _, _ = other(lax.rem(tz - z + depth, depth), dy, dx)
                        if i < shelf:
                            send_tokens(there * 2 + 1)
                        else:

                            @pl.when(jnp.logical_not(low) & (there != chip))
                            def _():
                                send_tokens(there * 2 + 1)

    with jax.named_scope("load_rest"):
        for load in loads:
            load.wait()

    def arrived(ref, semaphore):
        pltpu.make_async_remote_copy(
            src_ref=ref,
            dst_ref=ref,
            send_sem=send_a,
            recv_sem=semaphore,
            device_id={"frame": partner},
            device_id_type=MESH,
        ).wait_recv()

    def departed(ref, semaphore):
        pltpu.make_async_remote_copy(
            src_ref=ref,
            dst_ref=ref,
            send_sem=semaphore,
            recv_sem=recv_x,
            device_id={"frame": partner},
            device_id_type=MESH,
        ).wait_send()

    def project(tokens, places, ask=True):
        tokens = tokens.astype(jnp.float32)
        normed = (quadratic_average_rescaling(tokens) * gain_ref[...].reshape(1, width)).astype(
            jnp.bfloat16
        )
        q = jnp.dot(normed, wq[...], preferred_element_type=jnp.float32) if ask else None
        k = jnp.dot(normed, wk[...], preferred_element_type=jnp.float32)
        v = jnp.dot(normed, wv[...], preferred_element_type=jnp.float32)
        for h in range(HEADS_WIN):
            c = slice(h * CHANNELS_PER_ATT, (h + 1) * CHANNELS_PER_ATT)
            ks = quadratic_average_rescaling(k[:, c]).astype(jnp.bfloat16)
            vs = v[:, c].astype(jnp.bfloat16)
            if ask:
                qs = (
                    quadratic_average_rescaling(q[:, c]) * sharp_ref[h] / math.sqrt(CHANNELS_PER_ATT)
                ).astype(jnp.bfloat16)
            for i, place in enumerate(places):
                a = slice(i * rows, (i + 1) * rows)
                b = slice(place * rows, (place + 1) * rows)
                k_rows[b, c] = ks[a]
                v_rows[b, c] = vs[a]
                if ask:
                    q_rows[b, c] = qs[a]

    def ids(first, count, axis):
        shape = (count, 1) if axis == 0 else (1, count)
        r = first + lax.broadcasted_iota(jnp.int32, shape, axis)
        owner = r // block
        inner = r - owner * block
        return owner * local_frames + inner // positions, inner % positions

    def attend(asking, keys, target):
        first, count = asking
        start, length = keys
        base = 2 * rows if start >= 2 * rows else 0
        t_row, p_row = ids(first - base, count, 0)
        t_col, p_col = ids(start - base, length, 1)
        offset = t_row - t_col
        inside = (p_row == p_col) & (offset >= 0) & (offset < WINDOW)
        a, b = slice(first, first + count), slice(start, start + length)
        heads = [slice(h * CHANNELS_PER_ATT, (h + 1) * CHANNELS_PER_ATT) for h in range(HEADS_WIN)]
        scores = [
            lax.dot_general(
                q_rows[a, c],
                k_rows[b, c],
                (((1,), (1,)), ((), ())),
                preferred_element_type=jnp.float32,
            )
            for c in heads
        ]
        weights = [softmax_bf16(s, inside) for s in scores]
        attended = [
            jnp.dot(w, v_rows[b, c], preferred_element_type=jnp.float32)
            for w, c in zip(weights, heads)
        ]
        for c, part in zip(heads, attended):
            target[:, :, c] = part.reshape(half, block, CHANNELS_PER_ATT).astype(jnp.bfloat16)

    def tokens_of(part):
        return gathered[part * half : (part + 1) * half].reshape(rows, width)

    def send_back(target):
        remote(outgoing.at[target], returned.at[side, chip], send_b, recv_b.at[side], target)

    def back_to_high():
        for k in range(half // 2):
            there = half // 2 + lax.rem(chip + k, half // 2)
            for s in range(2):
                target = there * 2 + s

                @pl.when(target != me)
                def _():
                    send_back(target)

    @pl.when(low)
    def _():
        with jax.named_scope("wait_own"):
            arrived(gathered.at[pl.ds(0, half - 1)], recv_a.at[0])
        with jax.named_scope("work_own"):
            project(tokens_of(0), (0,))
            attend((0, rows), (0, rows), outgoing.at[pl.ds(0, half)])
            for k in range(1, half):
                send_back(lax.rem(me + k, half))
            returned[side, chip] = outgoing[me]
        def extras():
            with jax.named_scope("wait_extra"):
                arrived(extra.at[pl.ds(0, half - 1)], recv_x)
            with jax.named_scope("work_extra"):
                project(extra[...].reshape(rows, width), (2,))
                attend((2 * rows, rows), (2 * rows, rows), outgoing_extra)
                for k in range(1, half):
                    target = lax.rem(me + k, half)
                    remote(
                        outgoing_extra.at[target],
                        returned.at[1, chip + half // 2],
                        send_c,
                        recv_b.at[1],
                        target,
                    )
                returned[1, chip + half // 2] = outgoing_extra[me]

        with jax.named_scope("wait_far"):
            arrived(gathered.at[pl.ds(0, half)], recv_a.at[1])
        with jax.named_scope("work_far"):
            project(tokens_of(1), (1,))
            attend((rows, rows), (0, 2 * rows), outgoing.at[pl.ds(half, half)])
            back_to_high()
        pl.when(side == 0)(extras)

    @pl.when(jnp.logical_not(low))
    def _():
        with jax.named_scope("wait_own"):
            arrived(gathered.at[pl.ds(0, half - 1)], recv_a.at[1])
        with jax.named_scope("work_own"):
            project(tokens_of(1), (1,))
        with jax.named_scope("wait_far"):
            arrived(gathered.at[pl.ds(0, half)], recv_a.at[0])

        @pl.when(side == 0)
        def _():
            with jax.named_scope("work_far"):
                project(tokens_of(0), (0,))
                attend((0, rows), (0, rows), outgoing.at[pl.ds(0, half)])
                for k in range(half):
                    send_back(lax.rem(me + k, half))
                attend((rows, rows), (0, 2 * rows), outgoing.at[pl.ds(half, half)])
                back_to_high()

        @pl.when(side == 1)
        def _():
            with jax.named_scope("work_far"):
                project(tokens_of(0), (0,), ask=False)
                attend((rows, rows), (0, 2 * rows), outgoing.at[pl.ds(half, half)])
                back_to_high()

        returned[side, chip] = outgoing[me]

    for s in range(2):
        with jax.named_scope(f"wait_b{s}"):
            fewer = (side == s) | low if s else side == s

            @pl.when(fewer)
            def _():
                arrived(returned.at[s, pl.ds(0, half - 1)], recv_b.at[s])

            @pl.when(jnp.logical_not(fewer))
            def _():
                arrived(returned.at[s], recv_b.at[s])

        with jax.named_scope(f"finish{s}"):
            if s:
                left_ref[...] = returned[s].reshape(rows, HIGH)
            else:
                summed = jnp.dot(
                    returned[s].reshape(rows, HIGH), wo[...], preferred_element_type=jnp.float32
                )
                for k in range(half):
                    done_ref[k] = (
                        summed[k * block : (k + 1) * block] + x_own[2 * k].astype(jnp.float32)
                    ).astype(jnp.bfloat16)

    with jax.named_scope("departed"):
        departed(x_own.at[pl.ds(0, devices - 1)], send_a)

        @pl.when(low & (side == 0))
        def _():
            departed(x_own.at[pl.ds(0, half // 2 - 1)], send_x)
            departed(outgoing_extra.at[pl.ds(0, half - 1)], send_c)

        @pl.when(low & (side == 1))
        def _():
            departed(x_own.at[pl.ds(0, half // 2)], send_x)

        @pl.when(low | (side == 0))
        def _():
            departed(outgoing.at[pl.ds(0, devices - 1)], send_b)

        @pl.when(jnp.logical_not(low) & (side == 1))
        def _():
            departed(outgoing.at[pl.ds(0, half - 1)], send_b)


def finish(done, left, x_own, wo, result, held, sem):
    half, block, width = done.shape
    first = pltpu.make_async_copy(done, result.at[:, 0], sem.at[0])
    first.start()
    pieces = sem.shape[0] - 1
    share = width // pieces
    copies = []
    for n in range(pieces):
        c = slice(n * share, (n + 1) * share)
        summed = jnp.dot(left[...], wo[:, c], preferred_element_type=jnp.float32)
        for k in range(half):
            held[k, :, c] = (
                summed[k * block : (k + 1) * block] + x_own[2 * k + 1, :, c].astype(jnp.float32)
            ).astype(jnp.bfloat16)
        copies.append(
            pltpu.make_async_copy(
                held.at[:, :, pl.ds(n * share, share)],
                result.at[:, 1, :, pl.ds(n * share, share)],
                sem.at[n + 1],
            )
        )
        copies[-1].start()
    first.wait()
    for copy in copies:
        copy.wait()


def local_fused(devices, x, gain, wq, wk, wv, sharp, wo):
    local_frames, seq_len, width = x.shape
    positions = seq_len // devices
    block = local_frames * positions
    half = devices // 2
    rows = half * block
    blocks = x.reshape(local_frames, devices, positions, width)
    blocks = blocks.transpose(1, 0, 2, 3).reshape(devices, block, width)
    vmem = pl.BlockSpec(memory_space=pltpu.VMEM)
    anywhere = pl.BlockSpec(memory_space=pl.ANY)
    dma = pltpu.SemaphoreType.DMA
    held = (half, block, width)
    parts = pl.pallas_call(
        functools.partial(fused, devices, local_frames),
        out_shape=[
            pltpu.VMEM(held, jnp.bfloat16),
            pltpu.VMEM((rows, HIGH), jnp.bfloat16),
            pltpu.VMEM(blocks.shape, jnp.bfloat16),
            pltpu.VMEM(wo.shape, jnp.bfloat16),
        ],
        in_specs=[anywhere] * 7,
        out_specs=[vmem] * 4,
        scratch_shapes=[
            pltpu.SMEM(sharp.shape, jnp.float32),
            pltpu.VMEM(gain.shape, jnp.float32),
            pltpu.VMEM(wq.shape, jnp.bfloat16),
            pltpu.VMEM(wk.shape, jnp.bfloat16),
            pltpu.VMEM(wv.shape, jnp.bfloat16),
            pltpu.VMEM(blocks.shape, jnp.bfloat16),
            pltpu.VMEM((half, block, width), jnp.bfloat16),
            pltpu.VMEM((3 * rows, HIGH), jnp.bfloat16),
            pltpu.VMEM((3 * rows, HIGH), jnp.bfloat16),
            pltpu.VMEM((3 * rows, HIGH), jnp.bfloat16),
            pltpu.VMEM((devices, block, HIGH), jnp.bfloat16),
            pltpu.VMEM((half, block, HIGH), jnp.bfloat16),
            pltpu.VMEM((2, half, block, HIGH), jnp.bfloat16),
            dma((7,)),
            pltpu.SemaphoreType.REGULAR((devices // 2,)),
            dma,
            dma,
            dma((2,)),
            dma,
            dma,
            dma,
            dma((2,)),
        ],
        compiler_params=pltpu.CompilerParams(
            collective_id=0, has_side_effects=True, vmem_limit_bytes=60 * 2**20
        ),
    )(sharp, blocks, gain, wq, wk, wv, wo)
    out = pl.pallas_call(
        finish,
        out_shape=jax.ShapeDtypeStruct((half, 2, block, width), jnp.bfloat16),
        in_specs=[vmem] * 4,
        out_specs=anywhere,
        scratch_shapes=[pltpu.VMEM(held, jnp.bfloat16), dma((3,))],
    )(*[pltpu.with_memory_space_constraint(part, pltpu.VMEM) for part in parts])
    out = out.reshape(devices, local_frames, positions, width).transpose(1, 0, 2, 3)
    return out.reshape(x.shape)


def solution(mesh):
    devices = mesh.shape["frame"]

    def body(x, *rest):
        positions = x.shape[1] // devices
        if devices % 16 == 0 and positions % 8 == 0:
            return local_fused(devices, x, *rest)
        return local(x, *rest)

    placed = (P(("clips", "frame"), None, None), P(), P(), P(), P(), P(), P())
    return jax.shard_map(
        body,
        mesh=mesh,
        in_specs=placed,
        out_specs=P(("clips", "frame"), None, None),
        check_vma=False,
    )
```

```python
import functools
import math

import jax
import jax.numpy as jnp
from jax import lax
from jax.experimental import pallas as pl
from jax.experimental.pallas import tpu as pltpu
from jax.sharding import PartitionSpec as P

HEADS_WIN = 5
CHANNELS_PER_ATT = 128
WINDOW = 32


epsilon = 1e-06


def quadratic_average_rescaling(values):
    return values * lax.rsqrt(jnp.mean(values * values, axis=-1, keepdims=True) + epsilon)


def project_through(
    incoming_token_vectors,
    asking_projection_tensor,
    lookup_projection_tensor,
    content_projection_tensor,
    logit_sharpness,
):
    lead = incoming_token_vectors.shape[:-1]
    flat_rows = incoming_token_vectors.reshape(-1, incoming_token_vectors.shape[-1])
    shape_heads = lead + (HEADS_WIN, CHANNELS_PER_ATT)
    asking_vectors_full = jnp.dot(
        flat_rows, asking_projection_tensor, preferred_element_type=jnp.float32
    ).reshape(shape_heads)
    k_full = jnp.dot(
        flat_rows, lookup_projection_tensor, preferred_element_type=jnp.float32
    ).reshape(shape_heads)
    v_full = jnp.dot(
        flat_rows, content_projection_tensor, preferred_element_type=jnp.float32
    ).reshape(shape_heads)
    asking_token_vectors = (
        quadratic_average_rescaling(asking_vectors_full)
        * logit_sharpness[:, None]
        / math.sqrt(CHANNELS_PER_ATT)
    ).astype(jnp.bfloat16)
    key_matrix_rows = quadratic_average_rescaling(k_full).astype(jnp.bfloat16)
    return (asking_token_vectors, key_matrix_rows, v_full.astype(jnp.bfloat16))


def softmax_bf16(scores, window_mask):
    scores = jnp.where(window_mask, scores, -1e30)
    top = jnp.max(scores, axis=-1, keepdims=True)
    expo = jnp.exp(scores - top)
    return (expo / jnp.sum(expo, axis=-1, keepdims=True)).astype(jnp.bfloat16)


def band_attention(asking_token_vectors, key_matrix_rows, value_matrix_rows):
    all_frames, positions, heads, width = asking_token_vectors.shape
    blocks = all_frames // WINDOW
    block_shape = (blocks, WINDOW, positions, heads, width)
    q_blocks = asking_token_vectors.reshape(block_shape)
    k_blocks = key_matrix_rows.reshape(block_shape)
    v_blocks = value_matrix_rows.reshape(block_shape)
    k_earlier = jnp.concatenate([jnp.zeros_like(k_blocks[:1]), k_blocks[:-1]], axis=0)
    v_earlier = jnp.concatenate([jnp.zeros_like(v_blocks[:1]), v_blocks[:-1]], axis=0)
    k_pair = jnp.concatenate([k_earlier, k_blocks], axis=1)
    v_pair = jnp.concatenate([v_earlier, v_blocks], axis=1)
    scores = jnp.einsum("bqphd,bkphd->bphqk", q_blocks, k_pair, preferred_element_type=jnp.float32)
    block_ids = jnp.arange(blocks, dtype=jnp.int32)[:, None, None]
    row_ids = jnp.arange(WINDOW, dtype=jnp.int32)[None, :, None]
    col_ids = jnp.arange(2 * WINDOW, dtype=jnp.int32)[None, None, :]
    offset = row_ids - col_ids + WINDOW
    inside = (offset >= 0) & (offset < WINDOW) & (block_ids * WINDOW - WINDOW + col_ids >= 0)
    weights = softmax_bf16(scores, inside[:, None, None])
    attended = jnp.einsum("bphqk,bkphd->bqphd", weights, v_pair, preferred_element_type=jnp.float32)
    return attended.astype(jnp.bfloat16).reshape(all_frames, positions, heads, width)


def local(
    frame_sequence_elements,
    entry_rescaling_factors,
    asking_projection_tensor,
    lookup_projection_tensor,
    content_projection_tensor,
    logit_sharpness,
    final_projection_tensor,
):
    frames_dev, seq_len, width = frame_sequence_elements.shape
    floated = frame_sequence_elements.astype(jnp.float32)
    rescaled_token_vectors = (
        quadratic_average_rescaling(floated) * entry_rescaling_factors
    ).astype(jnp.bfloat16)
    position_rows = lax.all_to_all(
        rescaled_token_vectors, "frame", split_axis=1, concat_axis=0, tiled=True
    )
    asking_token_vectors, key_matrix_rows, value_matrix_rows = project_through(
        position_rows,
        asking_projection_tensor,
        lookup_projection_tensor,
        content_projection_tensor,
        logit_sharpness,
    )
    result = band_attention(asking_token_vectors, key_matrix_rows, value_matrix_rows)
    attended = lax.all_to_all(result, "frame", split_axis=0, concat_axis=1, tiled=True)
    flat_attended = attended.reshape(frames_dev * seq_len, -1)
    summed = jnp.dot(
        flat_attended, final_projection_tensor, preferred_element_type=jnp.float32
    ) + floated.reshape(frames_dev * seq_len, width)
    return summed.astype(jnp.bfloat16).reshape(frames_dev, seq_len, width)


MESH = pl.DeviceIdType.MESH
HIGH = HEADS_WIN * CHANNELS_PER_ATT


def fused(
    devices,
    local_frames,
    sharp_hbm,
    x_hbm,
    gain_hbm,
    wq_hbm,
    wk_hbm,
    wv_hbm,
    wo_hbm,
    done_ref,
    left_ref,
    x_own,
    wo,
    sharp_ref,
    gain_ref,
    wq,
    wk,
    wv,
    gathered,
    extra,
    q_rows,
    k_rows,
    v_rows,
    outgoing,
    outgoing_extra,
    returned,
    load_sem,
    ready,
    send_a,
    send_x,
    recv_a,
    recv_x,
    send_b,
    send_c,
    recv_b,
):
    me = lax.axis_index("frame")
    block, width = x_own.shape[1], x_own.shape[2]
    positions = block // local_frames
    chips = devices // 2
    depth = chips // 4
    half = devices // 2
    rows = half * block
    chip, side = me // 2, lax.rem(me, 2)
    partner = me + 1 - 2 * side
    z, y, x = chip // 4, lax.rem(chip // 2, 2), lax.rem(chip, 2)
    low = me < half

    def other(dz, dy, dx):
        tz = lax.rem(z + dz, depth)
        ty = y + dy - 2 * dy * y
        tx = x + dx - 2 * dx * x
        above = (tz >= z) & (ty >= y) & (tx >= x)
        below = (tz <= z) & (ty <= y) & (tx <= x)
        return tz * 4 + ty * 2 + tx, above, below

    steps = [(dz, dy, dx) for dz in range(depth) for dy in range(2) for dx in range(2)][1:]
    far_first = sorted(steps, key=lambda s: (s[0] == 0, s[0]))
    near_first = sorted(steps, key=lambda s: (sum(s), s[0]))

    x_load = pltpu.make_async_copy(x_hbm, x_own, load_sem.at[0])
    x_load.start()
    barrier = pltpu.get_barrier_semaphore()

    def signal(semaphore, target):
        pl.semaphore_signal(
            semaphore, inc=1, device_id={"frame": target}, device_id_type=MESH
        )

    signal(barrier, partner)
    for step in near_first:
        there, above, _ = other(*step)

        @pl.when(above)
        def _():
            signal(barrier, there * 2)
            signal(barrier, there * 2 + 1)

    loads = [
        pltpu.make_async_copy(source, target, load_sem.at[i + 1])
        for i, (source, target) in enumerate(
            (
                (sharp_hbm, sharp_ref),
                (gain_hbm, gain_ref),
                (wq_hbm, wq),
                (wk_hbm, wk),
                (wv_hbm, wv),
                (wo_hbm, wo),
            )
        )
    ]
    for load in loads:
        load.start()
    with jax.named_scope("barrier"):
        pl.semaphore_wait(barrier, 2 * ((z + 1) * (y + 1) * (x + 1) - 1) + 1)
    for step in far_first:
        there, _, below = other(*step)

        @pl.when(below)
        def _():
            signal(ready.at[chip], there * 2)
            signal(ready.at[chip], there * 2 + 1)

    with jax.named_scope("load_x"):
        x_load.wait()

    def remote(source, target, send, recv, device):
        pltpu.make_async_remote_copy(
            src_ref=source,
            dst_ref=target,
            send_sem=send,
            recv_sem=recv,
            device_id={"frame": device},
            device_id_type=MESH,
        ).start()

    layer = devices // depth
    layer_rows = layer * block

    def send_tokens(target):
        remote(x_own.at[target], gathered.at[me], send_a, recv_a.at[z], target)

    def send_extra(target):
        remote(x_own.at[target + 1 + half], extra.at[me], send_x, recv_x, target)

    shelf = depth // 2
    inner = z < shelf - 1

    def send_four(there):
        for s in range(2):
            send_tokens(there * 2 + s)
        send_extra(there * 2)

    with jax.named_scope("send_first"):
        send_tokens(partner)

        @pl.when(low & (side == 1))
        def _():
            send_extra(partner)

        @pl.when(low & (side == 0))
        def _():
            extra[me] = x_own[me + 1 + half]

        gathered[me] = x_own[me]

    def plane(step):
        return lax.rem(z + step[0], depth)

    def each_below(act):
        for step in far_first:
            there, _, below = other(*step)
            pl.when(below)(functools.partial(act, there))

    def each_joined(wanted, act):
        for step in near_first:
            dz, dy, dx = step
            there, above, _ = other(*step)

            @pl.when(above & wanted(step))
            def _():
                pl.semaphore_wait(ready.at[there], 2)
                act(there, step)
                ty, tx = lax.rem(there // 2, 2), lax.rem(there, 2)
                for p in range(depth) if dz == 0 else (None,):
                    tz = there // 4 if p is None else p
                    for ey in range(2 - dy):
                        for ex in range(2 - dx):
                            found = (y >= ey) & (x >= ex)
                            if p is not None:
                                found &= (p < z) | ((p == z) & (ey + ex > 0))
                            elif ey + ex == 0:
                                continue
                            pl.when(found)(
                                functools.partial(
                                    act, tz * 4 + (ty - ey) * 2 + tx - ex, step
                                )
                            )

    @pl.when(inner)
    def _():
        with jax.named_scope("send_group"):
            each_below(send_four)
            each_joined(lambda step: plane(step) < shelf, lambda there, step: send_four(there))

        with jax.named_scope("send_across"):
            each_joined(
                lambda step: plane(step) >= shelf, lambda there, step: send_tokens(there * 2)
            )
            for step in near_first:
                there, _, _ = other(*step)

                @pl.when(plane(step) >= shelf)
                def _():
                    send_tokens(there * 2 + 1)

    @pl.when(jnp.logical_not(inner))
    def _():
        with jax.named_scope("send_below"):
            each_below(lambda there: send_tokens(there * 2))

        with jax.named_scope("send_above"):
            each_joined(lambda step: True, lambda there, step: send_tokens(there * 2))

        with jax.named_scope("send_rest"):

            @pl.when(low)
            def _():
                for k in range(1, half // 2):
                    there = lax.rem(chip + k, half // 2)
                    send_tokens(there * 2 + 1)
                    send_extra(there * 2)

            for i in range(depth):
                upward = jnp.where(z == depth - 1, (i + shelf) % depth, i)
                tz = jnp.where(low, (i + shelf) % depth, upward)
                for dy in range(2):
                    for dx in range(2):
                        there, _, _ = other(lax.rem(tz - z + depth, depth), dy, dx)

                        @pl.when((there != chip) & (jnp.logical_not(low) | (tz >= shelf)))
                        def _():
                            send_tokens(there * 2 + 1)

    with jax.named_scope("load_rest"):
        for load in loads:
            load.wait()

    def arrived(ref, semaphore):
        pltpu.make_async_remote_copy(
            src_ref=ref,
            dst_ref=ref,
            send_sem=send_a,
            recv_sem=semaphore,
            device_id={"frame": partner},
            device_id_type=MESH,
        ).wait_recv()

    def departed(ref, semaphore):
        pltpu.make_async_remote_copy(
            src_ref=ref,
            dst_ref=ref,
            send_sem=semaphore,
            recv_sem=recv_x,
            device_id={"frame": partner},
            device_id_type=MESH,
        ).wait_send()

    def project(tokens, place, ask=True):
        tokens = tokens.reshape(-1, width).astype(jnp.float32)
        normed = (quadratic_average_rescaling(tokens) * gain_ref[...].reshape(1, width)).astype(
            jnp.bfloat16
        )
        q = jnp.dot(normed, wq[...], preferred_element_type=jnp.float32) if ask else None
        k = jnp.dot(normed, wk[...], preferred_element_type=jnp.float32)
        v = jnp.dot(normed, wv[...], preferred_element_type=jnp.float32)
        b = slice(place, place + tokens.shape[0])
        for h in range(HEADS_WIN):
            c = slice(h * CHANNELS_PER_ATT, (h + 1) * CHANNELS_PER_ATT)
            if ask:
                q_rows[b, c] = (
                    quadratic_average_rescaling(q[:, c]) * sharp_ref[h] / math.sqrt(CHANNELS_PER_ATT)
                ).astype(jnp.bfloat16)
            k_rows[b, c] = quadratic_average_rescaling(k[:, c]).astype(jnp.bfloat16)
            v_rows[b, c] = v[:, c].astype(jnp.bfloat16)

    def ids(first, count, axis):
        shape = (count, 1) if axis == 0 else (1, count)
        r = first + lax.broadcasted_iota(jnp.int32, shape, axis)
        owner = r // block
        inner = r - owner * block
        return owner * local_frames + inner // positions, inner % positions

    def attend(asking, keys, target):
        first, count = asking
        start, length = keys
        base = 2 * rows if start >= 2 * rows else 0
        t_row, p_row = ids(first - base, count, 0)
        t_col, p_col = ids(start - base, length, 1)
        offset = t_row - t_col
        inside = (p_row == p_col) & (offset >= 0) & (offset < WINDOW)
        a, b = slice(first, first + count), slice(start, start + length)
        heads = [slice(h * CHANNELS_PER_ATT, (h + 1) * CHANNELS_PER_ATT) for h in range(HEADS_WIN)]
        scores = [
            lax.dot_general(
                q_rows[a, c],
                k_rows[b, c],
                (((1,), (1,)), ((), ())),
                preferred_element_type=jnp.float32,
            )
            for c in heads
        ]
        weights = [softmax_bf16(s, inside) for s in scores]
        attended = [
            jnp.dot(w, v_rows[b, c], preferred_element_type=jnp.float32)
            for w, c in zip(weights, heads)
        ]
        for c, part in zip(heads, attended):
            target[:, :, c] = part.reshape(count // block, block, CHANNELS_PER_ATT).astype(
                jnp.bfloat16
            )

    def send_back(target):
        remote(outgoing.at[target], returned.at[side, chip], send_b, recv_b.at[side], target)

    def back_to_layer(p):
        for k in range(layer // 2):
            there = p * (layer // 2) + lax.rem(chip + k, layer // 2)
            for s in range(2):
                target = there * 2 + s

                @pl.when(target != me)
                def _():
                    send_back(target)

    def wait_layer(p):
        @pl.when(z == p)
        def _():
            arrived(gathered.at[pl.ds(0, layer - 1)], recv_a.at[p])

        @pl.when(z != p)
        def _():
            arrived(gathered.at[pl.ds(0, layer)], recv_a.at[p])

    lower, upper = range(shelf), range(shelf, depth)

    @pl.when(low)
    def _():
        with jax.named_scope("wait_own"):
            for p in lower:
                wait_layer(p)
        with jax.named_scope("work_own"):
            project(gathered[:half], 0)
            attend((0, rows), (0, rows), outgoing.at[pl.ds(0, half)])
            for k in range(1, half):
                send_back(lax.rem(me + k, half))
            returned[side, chip] = outgoing[me]

        for p in upper:
            with jax.named_scope(f"wait_far{p}"):
                wait_layer(p)
            with jax.named_scope(f"work_far{p}"):
                project(gathered[p * layer : (p + 1) * layer], p * layer_rows)
                attend(
                    (p * layer_rows, layer_rows),
                    (0, (p + 1) * layer_rows),
                    outgoing.at[pl.ds(p * layer, layer)],
                )
                back_to_layer(p)

        @pl.when(side == 0)
        def _():
            with jax.named_scope("wait_extra"):
                arrived(extra.at[pl.ds(0, half - 1)], recv_x)
            with jax.named_scope("work_extra"):
                project(extra[...], 2 * rows)
                attend((2 * rows, rows), (2 * rows, rows), outgoing_extra)
                for k in range(1, half):
                    target = lax.rem(me + k, half)
                    remote(
                        outgoing_extra.at[target],
                        returned.at[1, chip + half // 2],
                        send_c,
                        recv_b.at[1],
                        target,
                    )
                returned[1, chip + half // 2] = outgoing_extra[me]

    @pl.when(jnp.logical_not(low))
    def _():
        with jax.named_scope("wait_own"):
            for p in upper:
                wait_layer(p)
        with jax.named_scope("work_own"):
            project(gathered[half:], rows)
        with jax.named_scope("wait_far"):
            for p in lower:
                wait_layer(p)

        @pl.when(side == 0)
        def _():
            with jax.named_scope("work_far"):
                project(gathered[:half], 0)
                attend((0, rows), (0, rows), outgoing.at[pl.ds(0, half)])
                for k in range(half):
                    send_back(lax.rem(me + k, half))
                attend((rows, rows), (0, 2 * rows), outgoing.at[pl.ds(half, half)])
                for p in upper:
                    back_to_layer(p)

        @pl.when(side == 1)
        def _():
            with jax.named_scope("work_far"):
                project(gathered[:half], 0, ask=False)
                attend((rows, rows), (0, 2 * rows), outgoing.at[pl.ds(half, half)])
                for p in upper:
                    back_to_layer(p)

        returned[side, chip] = outgoing[me]

    for s in range(2):
        with jax.named_scope(f"wait_b{s}"):
            fewer = (side == s) | low if s else side == s

            @pl.when(fewer)
            def _():
                arrived(returned.at[s, pl.ds(0, half - 1)], recv_b.at[s])

            @pl.when(jnp.logical_not(fewer))
            def _():
                arrived(returned.at[s], recv_b.at[s])

        with jax.named_scope(f"finish{s}"):
            if s:
                left_ref[...] = returned[s].reshape(rows, HIGH)
            else:
                summed = jnp.dot(
                    returned[s].reshape(rows, HIGH), wo[...], preferred_element_type=jnp.float32
                )
                for k in range(half):
                    done_ref[k] = (
                        summed[k * block : (k + 1) * block] + x_own[2 * k].astype(jnp.float32)
                    ).astype(jnp.bfloat16)

    with jax.named_scope("departed"):
        departed(x_own.at[pl.ds(0, devices - 1)], send_a)

        @pl.when(low & (side == 0))
        def _():
            departed(x_own.at[pl.ds(0, half // 2 - 1)], send_x)
            departed(outgoing_extra.at[pl.ds(0, half - 1)], send_c)

        @pl.when(low & (side == 1))
        def _():
            departed(x_own.at[pl.ds(0, half // 2)], send_x)

        @pl.when(low | (side == 0))
        def _():
            departed(outgoing.at[pl.ds(0, devices - 1)], send_b)

        @pl.when(jnp.logical_not(low) & (side == 1))
        def _():
            departed(outgoing.at[pl.ds(0, half - 1)], send_b)


def finish(done, left, x_own, wo, result, held, sem):
    half, block, width = done.shape
    first = pltpu.make_async_copy(done, result.at[:, 0], sem.at[0])
    first.start()
    pieces = sem.shape[0] - 1
    share = width // pieces
    copies = []
    for n in range(pieces):
        c = slice(n * share, (n + 1) * share)
        summed = jnp.dot(left[...], wo[:, c], preferred_element_type=jnp.float32)
        for k in range(half):
            held[k, :, c] = (
                summed[k * block : (k + 1) * block] + x_own[2 * k + 1, :, c].astype(jnp.float32)
            ).astype(jnp.bfloat16)
        copies.append(
            pltpu.make_async_copy(
                held.at[:, :, pl.ds(n * share, share)],
                result.at[:, 1, :, pl.ds(n * share, share)],
                sem.at[n + 1],
            )
        )
        copies[-1].start()
    first.wait()
    for copy in copies:
        copy.wait()


def local_fused(devices, x, gain, wq, wk, wv, sharp, wo):
    local_frames, seq_len, width = x.shape
    positions = seq_len // devices
    block = local_frames * positions
    half = devices // 2
    rows = half * block
    blocks = x.reshape(local_frames, devices, positions, width)
    blocks = blocks.transpose(1, 0, 2, 3).reshape(devices, block, width)
    vmem = pl.BlockSpec(memory_space=pltpu.VMEM)
    anywhere = pl.BlockSpec(memory_space=pl.ANY)
    dma = pltpu.SemaphoreType.DMA
    held = (half, block, width)
    parts = pl.pallas_call(
        functools.partial(fused, devices, local_frames),
        out_shape=[
            pltpu.VMEM(held, jnp.bfloat16),
            pltpu.VMEM((rows, HIGH), jnp.bfloat16),
            pltpu.VMEM(blocks.shape, jnp.bfloat16),
            pltpu.VMEM(wo.shape, jnp.bfloat16),
        ],
        in_specs=[anywhere] * 7,
        out_specs=[vmem] * 4,
        scratch_shapes=[
            pltpu.SMEM(sharp.shape, jnp.float32),
            pltpu.VMEM(gain.shape, jnp.float32),
            pltpu.VMEM(wq.shape, jnp.bfloat16),
            pltpu.VMEM(wk.shape, jnp.bfloat16),
            pltpu.VMEM(wv.shape, jnp.bfloat16),
            pltpu.VMEM(blocks.shape, jnp.bfloat16),
            pltpu.VMEM((half, block, width), jnp.bfloat16),
            pltpu.VMEM((3 * rows, HIGH), jnp.bfloat16),
            pltpu.VMEM((3 * rows, HIGH), jnp.bfloat16),
            pltpu.VMEM((3 * rows, HIGH), jnp.bfloat16),
            pltpu.VMEM((devices, block, HIGH), jnp.bfloat16),
            pltpu.VMEM((half, block, HIGH), jnp.bfloat16),
            pltpu.VMEM((2, half, block, HIGH), jnp.bfloat16),
            dma((7,)),
            pltpu.SemaphoreType.REGULAR((devices // 2,)),
            dma,
            dma,
            dma((devices // 8,)),
            dma,
            dma,
            dma,
            dma((2,)),
        ],
        compiler_params=pltpu.CompilerParams(
            collective_id=0, has_side_effects=True, vmem_limit_bytes=60 * 2**20
        ),
    )(sharp, blocks, gain, wq, wk, wv, wo)
    out = pl.pallas_call(
        finish,
        out_shape=jax.ShapeDtypeStruct((half, 2, block, width), jnp.bfloat16),
        in_specs=[vmem] * 4,
        out_specs=anywhere,
        scratch_shapes=[pltpu.VMEM(held, jnp.bfloat16), dma((3,))],
    )(*[pltpu.with_memory_space_constraint(part, pltpu.VMEM) for part in parts])
    out = out.reshape(devices, local_frames, positions, width).transpose(1, 0, 2, 3)
    return out.reshape(x.shape)


def solution(mesh):
    devices = mesh.shape["frame"]

    def body(x, *rest):
        positions = x.shape[1] // devices
        if devices % 16 == 0 and positions % 8 == 0:
            return local_fused(devices, x, *rest)
        return local(x, *rest)

    placed = (P(("clips", "frame"), None, None), P(), P(), P(), P(), P(), P())
    return jax.shard_map(
        body,
        mesh=mesh,
        in_specs=placed,
        out_specs=P(("clips", "frame"), None, None),
        check_vma=False,
    )
```

```python
import functools
import math

import jax
import jax.numpy as jnp
from jax import lax
from jax.experimental import pallas as pl
from jax.experimental.pallas import tpu as pltpu
from jax.sharding import PartitionSpec as P

HEADS_WIN = 5
CHANNELS_PER_ATT = 128
WINDOW = 32


epsilon = 1e-06


def quadratic_average_rescaling(values):
    return values * lax.rsqrt(jnp.mean(values * values, axis=-1, keepdims=True) + epsilon)


def project_through(
    incoming_token_vectors,
    asking_projection_tensor,
    lookup_projection_tensor,
    content_projection_tensor,
    logit_sharpness,
):
    lead = incoming_token_vectors.shape[:-1]
    flat_rows = incoming_token_vectors.reshape(-1, incoming_token_vectors.shape[-1])
    shape_heads = lead + (HEADS_WIN, CHANNELS_PER_ATT)
    asking_vectors_full = jnp.dot(
        flat_rows, asking_projection_tensor, preferred_element_type=jnp.float32
    ).reshape(shape_heads)
    k_full = jnp.dot(
        flat_rows, lookup_projection_tensor, preferred_element_type=jnp.float32
    ).reshape(shape_heads)
    v_full = jnp.dot(
        flat_rows, content_projection_tensor, preferred_element_type=jnp.float32
    ).reshape(shape_heads)
    asking_token_vectors = (
        quadratic_average_rescaling(asking_vectors_full)
        * logit_sharpness[:, None]
        / math.sqrt(CHANNELS_PER_ATT)
    ).astype(jnp.bfloat16)
    key_matrix_rows = quadratic_average_rescaling(k_full).astype(jnp.bfloat16)
    return (asking_token_vectors, key_matrix_rows, v_full.astype(jnp.bfloat16))


def softmax_bf16(scores, window_mask):
    scores = jnp.where(window_mask, scores, -1e30)
    top = jnp.max(scores, axis=-1, keepdims=True)
    expo = jnp.exp(scores - top)
    return (expo / jnp.sum(expo, axis=-1, keepdims=True)).astype(jnp.bfloat16)


def band_attention(asking_token_vectors, key_matrix_rows, value_matrix_rows):
    all_frames, positions, heads, width = asking_token_vectors.shape
    blocks = all_frames // WINDOW
    block_shape = (blocks, WINDOW, positions, heads, width)
    q_blocks = asking_token_vectors.reshape(block_shape)
    k_blocks = key_matrix_rows.reshape(block_shape)
    v_blocks = value_matrix_rows.reshape(block_shape)
    k_earlier = jnp.concatenate([jnp.zeros_like(k_blocks[:1]), k_blocks[:-1]], axis=0)
    v_earlier = jnp.concatenate([jnp.zeros_like(v_blocks[:1]), v_blocks[:-1]], axis=0)
    k_pair = jnp.concatenate([k_earlier, k_blocks], axis=1)
    v_pair = jnp.concatenate([v_earlier, v_blocks], axis=1)
    scores = jnp.einsum("bqphd,bkphd->bphqk", q_blocks, k_pair, preferred_element_type=jnp.float32)
    block_ids = jnp.arange(blocks, dtype=jnp.int32)[:, None, None]
    row_ids = jnp.arange(WINDOW, dtype=jnp.int32)[None, :, None]
    col_ids = jnp.arange(2 * WINDOW, dtype=jnp.int32)[None, None, :]
    offset = row_ids - col_ids + WINDOW
    inside = (offset >= 0) & (offset < WINDOW) & (block_ids * WINDOW - WINDOW + col_ids >= 0)
    weights = softmax_bf16(scores, inside[:, None, None])
    attended = jnp.einsum("bphqk,bkphd->bqphd", weights, v_pair, preferred_element_type=jnp.float32)
    return attended.astype(jnp.bfloat16).reshape(all_frames, positions, heads, width)


def local(
    frame_sequence_elements,
    entry_rescaling_factors,
    asking_projection_tensor,
    lookup_projection_tensor,
    content_projection_tensor,
    logit_sharpness,
    final_projection_tensor,
):
    frames_dev, seq_len, width = frame_sequence_elements.shape
    floated = frame_sequence_elements.astype(jnp.float32)
    rescaled_token_vectors = (
        quadratic_average_rescaling(floated) * entry_rescaling_factors
    ).astype(jnp.bfloat16)
    position_rows = lax.all_to_all(
        rescaled_token_vectors, "frame", split_axis=1, concat_axis=0, tiled=True
    )
    asking_token_vectors, key_matrix_rows, value_matrix_rows = project_through(
        position_rows,
        asking_projection_tensor,
        lookup_projection_tensor,
        content_projection_tensor,
        logit_sharpness,
    )
    result = band_attention(asking_token_vectors, key_matrix_rows, value_matrix_rows)
    attended = lax.all_to_all(result, "frame", split_axis=0, concat_axis=1, tiled=True)
    flat_attended = attended.reshape(frames_dev * seq_len, -1)
    summed = jnp.dot(
        flat_attended, final_projection_tensor, preferred_element_type=jnp.float32
    ) + floated.reshape(frames_dev * seq_len, width)
    return summed.astype(jnp.bfloat16).reshape(frames_dev, seq_len, width)


MESH = pl.DeviceIdType.MESH
HIGH = HEADS_WIN * CHANNELS_PER_ATT


def fused(
    devices,
    local_frames,
    sharp_hbm,
    x_hbm,
    gain_hbm,
    wq_hbm,
    wk_hbm,
    wv_hbm,
    wo_hbm,
    done_ref,
    left_ref,
    x_own,
    wo,
    sharp_ref,
    gain_ref,
    wq,
    wk,
    wv,
    gathered,
    extra,
    q_rows,
    k_rows,
    v_rows,
    outgoing,
    outgoing_extra,
    returned,
    load_sem,
    ready,
    send_a,
    send_x,
    recv_a,
    recv_x,
    send_b,
    send_c,
    recv_b,
):
    me = lax.axis_index("frame")
    block, width = x_own.shape[1], x_own.shape[2]
    positions = block // local_frames
    chips = devices // 2
    depth = chips // 4
    half = devices // 2
    rows = half * block
    chip, side = me // 2, lax.rem(me, 2)
    partner = me + 1 - 2 * side
    z, y, x = chip // 4, lax.rem(chip // 2, 2), lax.rem(chip, 2)
    low = me < half

    def other(dz, dy, dx):
        tz = lax.rem(z + dz, depth)
        ty = y + dy - 2 * dy * y
        tx = x + dx - 2 * dx * x
        above = (tz >= z) & (ty >= y) & (tx >= x)
        below = (tz <= z) & (ty <= y) & (tx <= x)
        return tz * 4 + ty * 2 + tx, above, below

    steps = [(dz, dy, dx) for dz in range(depth) for dy in range(2) for dx in range(2)][1:]
    far_first = sorted(steps, key=lambda s: (s[0] == 0, s[0]))
    near_first = sorted(steps, key=lambda s: (sum(s), s[0]))

    x_load = pltpu.make_async_copy(x_hbm, x_own, load_sem.at[0])
    x_load.start()
    barrier = pltpu.get_barrier_semaphore()

    def signal(semaphore, target):
        pl.semaphore_signal(
            semaphore, inc=1, device_id={"frame": target}, device_id_type=MESH
        )

    signal(barrier, partner)
    for step in near_first:
        there, above, _ = other(*step)

        @pl.when(above)
        def _():
            signal(barrier, there * 2)
            signal(barrier, there * 2 + 1)

    loads = [
        pltpu.make_async_copy(source, target, load_sem.at[i + 1])
        for i, (source, target) in enumerate(
            (
                (sharp_hbm, sharp_ref),
                (gain_hbm, gain_ref),
                (wq_hbm, wq),
                (wk_hbm, wk),
                (wv_hbm, wv),
                (wo_hbm, wo),
            )
        )
    ]
    for load in loads:
        load.start()
    with jax.named_scope("barrier"):
        pl.semaphore_wait(barrier, 2 * ((z + 1) * (y + 1) * (x + 1) - 1) + 1)
    for step in far_first:
        there, _, below = other(*step)

        @pl.when(below)
        def _():
            signal(ready.at[chip], there * 2)
            signal(ready.at[chip], there * 2 + 1)

    with jax.named_scope("load_x"):
        x_load.wait()

    def remote(source, target, send, recv, device):
        pltpu.make_async_remote_copy(
            src_ref=source,
            dst_ref=target,
            send_sem=send,
            recv_sem=recv,
            device_id={"frame": device},
            device_id_type=MESH,
        ).start()

    layer = devices // depth
    layer_rows = layer * block

    def send_tokens(target):
        remote(x_own.at[target], gathered.at[me], send_a, recv_a.at[z], target)

    def send_extra(target):
        remote(x_own.at[target + 1 + half], extra.at[me], send_x, recv_x, target)

    shelf = depth // 2
    inner = z < shelf - 1

    def send_four(there):
        for s in range(2):
            send_tokens(there * 2 + s)
        send_extra(there * 2)

    with jax.named_scope("send_first"):
        send_tokens(partner)

        @pl.when(low & (side == 1))
        def _():
            send_extra(partner)

        @pl.when(low & (side == 0))
        def _():
            extra[me] = x_own[me + 1 + half]

        gathered[me] = x_own[me]

    def plane(step):
        return lax.rem(z + step[0], depth)

    def each_below(act):
        for step in far_first:
            there, _, below = other(*step)
            pl.when(below)(functools.partial(act, there))

    def each_joined(wanted, act):
        for step in near_first:
            dz, dy, dx = step
            there, above, _ = other(*step)

            @pl.when(above & wanted(step))
            def _():
                pl.semaphore_wait(ready.at[there], 2)
                act(there, step)
                ty, tx = lax.rem(there // 2, 2), lax.rem(there, 2)
                for p in range(depth) if dz == 0 else (None,):
                    tz = there // 4 if p is None else p
                    for ey in range(2 - dy):
                        for ex in range(2 - dx):
                            found = (y >= ey) & (x >= ex)
                            if p is not None:
                                found &= (p < z) | ((p == z) & (ey + ex > 0))
                            elif ey + ex == 0:
                                continue
                            pl.when(found)(
                                functools.partial(
                                    act, tz * 4 + (ty - ey) * 2 + tx - ex, step
                                )
                            )

    @pl.when(inner)
    def _():
        with jax.named_scope("send_group"):
            each_below(send_four)
            each_joined(lambda step: plane(step) < shelf, lambda there, step: send_four(there))

        with jax.named_scope("send_across"):
            each_joined(
                lambda step: plane(step) >= shelf, lambda there, step: send_tokens(there * 2)
            )
            for step in near_first:
                there, _, _ = other(*step)

                @pl.when(plane(step) >= shelf)
                def _():
                    send_tokens(there * 2 + 1)

    @pl.when(jnp.logical_not(inner))
    def _():
        with jax.named_scope("send_below"):
            each_below(lambda there: send_tokens(there * 2))

        with jax.named_scope("send_above"):
            each_joined(lambda step: True, lambda there, step: send_tokens(there * 2))

        with jax.named_scope("send_rest"):

            @pl.when(low)
            def _():
                for k in range(1, half // 2):
                    there = lax.rem(chip + k, half // 2)
                    send_tokens(there * 2 + 1)
                    send_extra(there * 2)

            for i in range(depth):
                upward = jnp.where(z == depth - 1, (i + shelf) % depth, i)
                tz = jnp.where(low, (i + shelf) % depth, upward)
                for dy in range(2):
                    for dx in range(2):
                        there, _, _ = other(lax.rem(tz - z + depth, depth), dy, dx)

                        @pl.when((there != chip) & (jnp.logical_not(low) | (tz >= shelf)))
                        def _():
                            send_tokens(there * 2 + 1)

    with jax.named_scope("load_rest"):
        for load in loads:
            load.wait()

    def arrived(ref, semaphore):
        pltpu.make_async_remote_copy(
            src_ref=ref,
            dst_ref=ref,
            send_sem=send_a,
            recv_sem=semaphore,
            device_id={"frame": partner},
            device_id_type=MESH,
        ).wait_recv()

    def departed(ref, semaphore):
        pltpu.make_async_remote_copy(
            src_ref=ref,
            dst_ref=ref,
            send_sem=semaphore,
            recv_sem=recv_x,
            device_id={"frame": partner},
            device_id_type=MESH,
        ).wait_send()

    def project(tokens, place, ask=True):
        tokens = tokens.reshape(-1, width).astype(jnp.float32)
        normed = (quadratic_average_rescaling(tokens) * gain_ref[...].reshape(1, width)).astype(
            jnp.bfloat16
        )
        q = jnp.dot(normed, wq[...], preferred_element_type=jnp.float32) if ask else None
        k = jnp.dot(normed, wk[...], preferred_element_type=jnp.float32)
        v = jnp.dot(normed, wv[...], preferred_element_type=jnp.float32)
        b = slice(place, place + tokens.shape[0])
        for h in range(HEADS_WIN):
            c = slice(h * CHANNELS_PER_ATT, (h + 1) * CHANNELS_PER_ATT)
            if ask:
                q_rows[b, c] = (
                    quadratic_average_rescaling(q[:, c]) * sharp_ref[h] / math.sqrt(CHANNELS_PER_ATT)
                ).astype(jnp.bfloat16)
            k_rows[b, c] = quadratic_average_rescaling(k[:, c]).astype(jnp.bfloat16)
            v_rows[b, c] = v[:, c].astype(jnp.bfloat16)

    def ids(first, count, axis):
        shape = (count, 1) if axis == 0 else (1, count)
        r = first + lax.broadcasted_iota(jnp.int32, shape, axis)
        owner = r // block
        inner = r - owner * block
        return owner * local_frames + inner // positions, inner % positions

    def attend(asking, keys, target):
        first, count = asking
        start, length = keys
        base = 2 * rows if start >= 2 * rows else 0
        t_row, p_row = ids(first - base, count, 0)
        t_col, p_col = ids(start - base, length, 1)
        offset = t_row - t_col
        inside = (p_row == p_col) & (offset >= 0) & (offset < WINDOW)
        a, b = slice(first, first + count), slice(start, start + length)
        heads = [slice(h * CHANNELS_PER_ATT, (h + 1) * CHANNELS_PER_ATT) for h in range(HEADS_WIN)]
        scores = [
            lax.dot_general(
                q_rows[a, c],
                k_rows[b, c],
                (((1,), (1,)), ((), ())),
                preferred_element_type=jnp.float32,
            )
            for c in heads
        ]
        weights = [softmax_bf16(s, inside) for s in scores]
        attended = [
            jnp.dot(w, v_rows[b, c], preferred_element_type=jnp.float32)
            for w, c in zip(weights, heads)
        ]
        for c, part in zip(heads, attended):
            target[:, :, c] = part.reshape(count // block, block, CHANNELS_PER_ATT).astype(
                jnp.bfloat16
            )

    def send_back(target):
        remote(outgoing.at[target], returned.at[side, chip], send_b, recv_b.at[side], target)

    def back_to_layer(p):
        for k in range(layer // 2):
            there = p * (layer // 2) + lax.rem(chip + k, layer // 2)
            for s in range(2):
                target = there * 2 + s

                @pl.when(target != me)
                def _():
                    send_back(target)

    def wait_layer(p):
        @pl.when(z == p)
        def _():
            arrived(gathered.at[pl.ds(0, layer - 1)], recv_a.at[p])

        @pl.when(z != p)
        def _():
            arrived(gathered.at[pl.ds(0, layer)], recv_a.at[p])

    lower, upper = range(shelf), range(shelf, depth)

    @pl.when(low)
    def _():
        with jax.named_scope("wait_own"):
            for p in lower:
                wait_layer(p)
        with jax.named_scope("work_own"):
            project(gathered[:half], 0)
            attend((0, rows), (0, rows), outgoing.at[pl.ds(0, half)])
            for k in range(1, half):
                send_back(lax.rem(me + k, half))
            returned[side, chip] = outgoing[me]

        for p in reversed(upper):
            with jax.named_scope(f"wait_far{p}"):
                wait_layer(p)
            with jax.named_scope(f"work_far{p}"):
                project(gathered[p * layer : (p + 1) * layer], p * layer_rows)
        with jax.named_scope("work_back"):
            attend((rows, rows), (0, 2 * rows), outgoing.at[pl.ds(half, half)])
            for k in range(layer // 2):
                for p in upper:
                    there = p * (layer // 2) + lax.rem(chip + k, layer // 2)
                    send_back(there * 2)
                    send_back(there * 2 + 1)

        @pl.when(side == 0)
        def _():
            with jax.named_scope("wait_extra"):
                arrived(extra.at[pl.ds(0, half - 1)], recv_x)
            with jax.named_scope("work_extra"):
                project(extra[...], 2 * rows)
                attend((2 * rows, rows), (2 * rows, rows), outgoing_extra)
                for k in range(1, half):
                    target = lax.rem(me + k, half)
                    remote(
                        outgoing_extra.at[target],
                        returned.at[1, chip + half // 2],
                        send_c,
                        recv_b.at[1],
                        target,
                    )
                returned[1, chip + half // 2] = outgoing_extra[me]

    @pl.when(jnp.logical_not(low))
    def _():
        with jax.named_scope("wait_own"):
            for p in upper:
                wait_layer(p)
        with jax.named_scope("work_own"):
            project(gathered[half:], rows)
        with jax.named_scope("wait_far"):
            for p in lower:
                wait_layer(p)

        @pl.when(side == 0)
        def _():
            with jax.named_scope("work_far"):
                project(gathered[:half], 0)
                attend((0, rows), (0, rows), outgoing.at[pl.ds(0, half)])
                for k in range(half):
                    send_back(lax.rem(me + k, half))
                attend((rows, rows), (0, 2 * rows), outgoing.at[pl.ds(half, half)])
                for p in upper:
                    back_to_layer(p)

        @pl.when(side == 1)
        def _():
            with jax.named_scope("work_far"):
                project(gathered[:half], 0, ask=False)
                attend((rows, rows), (0, 2 * rows), outgoing.at[pl.ds(half, half)])
                for p in upper:
                    back_to_layer(p)

        returned[side, chip] = outgoing[me]

    for s in range(2):
        with jax.named_scope(f"wait_b{s}"):
            fewer = (side == s) | low if s else side == s

            @pl.when(fewer)
            def _():
                arrived(returned.at[s, pl.ds(0, half - 1)], recv_b.at[s])

            @pl.when(jnp.logical_not(fewer))
            def _():
                arrived(returned.at[s], recv_b.at[s])

        with jax.named_scope(f"finish{s}"):
            if s:
                left_ref[...] = returned[s].reshape(rows, HIGH)
            else:
                summed = jnp.dot(
                    returned[s].reshape(rows, HIGH), wo[...], preferred_element_type=jnp.float32
                )
                for k in range(half):
                    done_ref[k] = (
                        summed[k * block : (k + 1) * block] + x_own[2 * k].astype(jnp.float32)
                    ).astype(jnp.bfloat16)

    with jax.named_scope("departed"):
        departed(x_own.at[pl.ds(0, devices - 1)], send_a)

        @pl.when(low & (side == 0))
        def _():
            departed(x_own.at[pl.ds(0, half // 2 - 1)], send_x)
            departed(outgoing_extra.at[pl.ds(0, half - 1)], send_c)

        @pl.when(low & (side == 1))
        def _():
            departed(x_own.at[pl.ds(0, half // 2)], send_x)

        @pl.when(low | (side == 0))
        def _():
            departed(outgoing.at[pl.ds(0, devices - 1)], send_b)

        @pl.when(jnp.logical_not(low) & (side == 1))
        def _():
            departed(outgoing.at[pl.ds(0, half - 1)], send_b)


def finish(done, left, x_own, wo, result, held, sem):
    half, block, width = done.shape
    first = pltpu.make_async_copy(done, result.at[:, 0], sem.at[0])
    first.start()
    pieces = sem.shape[0] - 1
    share = width // pieces
    copies = []
    for n in range(pieces):
        c = slice(n * share, (n + 1) * share)
        summed = jnp.dot(left[...], wo[:, c], preferred_element_type=jnp.float32)
        for k in range(half):
            held[k, :, c] = (
                summed[k * block : (k + 1) * block] + x_own[2 * k + 1, :, c].astype(jnp.float32)
            ).astype(jnp.bfloat16)
        copies.append(
            pltpu.make_async_copy(
                held.at[:, :, pl.ds(n * share, share)],
                result.at[:, 1, :, pl.ds(n * share, share)],
                sem.at[n + 1],
            )
        )
        copies[-1].start()
    first.wait()
    for copy in copies:
        copy.wait()


def local_fused(devices, x, gain, wq, wk, wv, sharp, wo):
    local_frames, seq_len, width = x.shape
    positions = seq_len // devices
    block = local_frames * positions
    half = devices // 2
    rows = half * block
    blocks = x.reshape(local_frames, devices, positions, width)
    blocks = blocks.transpose(1, 0, 2, 3).reshape(devices, block, width)
    vmem = pl.BlockSpec(memory_space=pltpu.VMEM)
    anywhere = pl.BlockSpec(memory_space=pl.ANY)
    dma = pltpu.SemaphoreType.DMA
    held = (half, block, width)
    parts = pl.pallas_call(
        functools.partial(fused, devices, local_frames),
        out_shape=[
            pltpu.VMEM(held, jnp.bfloat16),
            pltpu.VMEM((rows, HIGH), jnp.bfloat16),
            pltpu.VMEM(blocks.shape, jnp.bfloat16),
            pltpu.VMEM(wo.shape, jnp.bfloat16),
        ],
        in_specs=[anywhere] * 7,
        out_specs=[vmem] * 4,
        scratch_shapes=[
            pltpu.SMEM(sharp.shape, jnp.float32),
            pltpu.VMEM(gain.shape, jnp.float32),
            pltpu.VMEM(wq.shape, jnp.bfloat16),
            pltpu.VMEM(wk.shape, jnp.bfloat16),
            pltpu.VMEM(wv.shape, jnp.bfloat16),
            pltpu.VMEM(blocks.shape, jnp.bfloat16),
            pltpu.VMEM((half, block, width), jnp.bfloat16),
            pltpu.VMEM((3 * rows, HIGH), jnp.bfloat16),
            pltpu.VMEM((3 * rows, HIGH), jnp.bfloat16),
            pltpu.VMEM((3 * rows, HIGH), jnp.bfloat16),
            pltpu.VMEM((devices, block, HIGH), jnp.bfloat16),
            pltpu.VMEM((half, block, HIGH), jnp.bfloat16),
            pltpu.VMEM((2, half, block, HIGH), jnp.bfloat16),
            dma((7,)),
            pltpu.SemaphoreType.REGULAR((devices // 2,)),
            dma,
            dma,
            dma((devices // 8,)),
            dma,
            dma,
            dma,
            dma((2,)),
        ],
        compiler_params=pltpu.CompilerParams(
            collective_id=0, has_side_effects=True, vmem_limit_bytes=60 * 2**20
        ),
    )(sharp, blocks, gain, wq, wk, wv, wo)
    out = pl.pallas_call(
        finish,
        out_shape=jax.ShapeDtypeStruct((half, 2, block, width), jnp.bfloat16),
        in_specs=[vmem] * 4,
        out_specs=anywhere,
        scratch_shapes=[pltpu.VMEM(held, jnp.bfloat16), dma((3,))],
    )(*[pltpu.with_memory_space_constraint(part, pltpu.VMEM) for part in parts])
    out = out.reshape(devices, local_frames, positions, width).transpose(1, 0, 2, 3)
    return out.reshape(x.shape)


def solution(mesh):
    devices = mesh.shape["frame"]

    def body(x, *rest):
        positions = x.shape[1] // devices
        if devices % 16 == 0 and positions % 8 == 0:
            return local_fused(devices, x, *rest)
        return local(x, *rest)

    placed = (P(("clips", "frame"), None, None), P(), P(), P(), P(), P(), P())
    return jax.shard_map(
        body,
        mesh=mesh,
        in_specs=placed,
        out_specs=P(("clips", "frame"), None, None),
        check_vma=False,
    )
```

```python
import functools
import math

import jax
import jax.numpy as jnp
from jax import lax
from jax.experimental import pallas as pl
from jax.experimental.pallas import tpu as pltpu
from jax.sharding import PartitionSpec as P

HEADS_WIN = 5
CHANNELS_PER_ATT = 128
WINDOW = 32


epsilon = 1e-06


def quadratic_average_rescaling(values):
    return values * lax.rsqrt(jnp.mean(values * values, axis=-1, keepdims=True) + epsilon)


def project_through(
    incoming_token_vectors,
    asking_projection_tensor,
    lookup_projection_tensor,
    content_projection_tensor,
    logit_sharpness,
):
    lead = incoming_token_vectors.shape[:-1]
    flat_rows = incoming_token_vectors.reshape(-1, incoming_token_vectors.shape[-1])
    shape_heads = lead + (HEADS_WIN, CHANNELS_PER_ATT)
    asking_vectors_full = jnp.dot(
        flat_rows, asking_projection_tensor, preferred_element_type=jnp.float32
    ).reshape(shape_heads)
    k_full = jnp.dot(
        flat_rows, lookup_projection_tensor, preferred_element_type=jnp.float32
    ).reshape(shape_heads)
    v_full = jnp.dot(
        flat_rows, content_projection_tensor, preferred_element_type=jnp.float32
    ).reshape(shape_heads)
    asking_token_vectors = (
        quadratic_average_rescaling(asking_vectors_full)
        * logit_sharpness[:, None]
        / math.sqrt(CHANNELS_PER_ATT)
    ).astype(jnp.bfloat16)
    key_matrix_rows = quadratic_average_rescaling(k_full).astype(jnp.bfloat16)
    return (asking_token_vectors, key_matrix_rows, v_full.astype(jnp.bfloat16))


def softmax_bf16(scores, window_mask):
    scores = jnp.where(window_mask, scores, -1e30)
    top = jnp.max(scores, axis=-1, keepdims=True)
    expo = jnp.exp(scores - top)
    return (expo * (1.0 / jnp.sum(expo, axis=-1, keepdims=True))).astype(jnp.bfloat16)


def band_attention(asking_token_vectors, key_matrix_rows, value_matrix_rows):
    all_frames, positions, heads, width = asking_token_vectors.shape
    blocks = all_frames // WINDOW
    block_shape = (blocks, WINDOW, positions, heads, width)
    q_blocks = asking_token_vectors.reshape(block_shape)
    k_blocks = key_matrix_rows.reshape(block_shape)
    v_blocks = value_matrix_rows.reshape(block_shape)
    k_earlier = jnp.concatenate([jnp.zeros_like(k_blocks[:1]), k_blocks[:-1]], axis=0)
    v_earlier = jnp.concatenate([jnp.zeros_like(v_blocks[:1]), v_blocks[:-1]], axis=0)
    k_pair = jnp.concatenate([k_earlier, k_blocks], axis=1)
    v_pair = jnp.concatenate([v_earlier, v_blocks], axis=1)
    scores = jnp.einsum("bqphd,bkphd->bphqk", q_blocks, k_pair, preferred_element_type=jnp.float32)
    block_ids = jnp.arange(blocks, dtype=jnp.int32)[:, None, None]
    row_ids = jnp.arange(WINDOW, dtype=jnp.int32)[None, :, None]
    col_ids = jnp.arange(2 * WINDOW, dtype=jnp.int32)[None, None, :]
    offset = row_ids - col_ids + WINDOW
    inside = (offset >= 0) & (offset < WINDOW) & (block_ids * WINDOW - WINDOW + col_ids >= 0)
    weights = softmax_bf16(scores, inside[:, None, None])
    attended = jnp.einsum("bphqk,bkphd->bqphd", weights, v_pair, preferred_element_type=jnp.float32)
    return attended.astype(jnp.bfloat16).reshape(all_frames, positions, heads, width)


def local(
    frame_sequence_elements,
    entry_rescaling_factors,
    asking_projection_tensor,
    lookup_projection_tensor,
    content_projection_tensor,
    logit_sharpness,
    final_projection_tensor,
):
    frames_dev, seq_len, width = frame_sequence_elements.shape
    floated = frame_sequence_elements.astype(jnp.float32)
    rescaled_token_vectors = (
        quadratic_average_rescaling(floated) * entry_rescaling_factors
    ).astype(jnp.bfloat16)
    position_rows = lax.all_to_all(
        rescaled_token_vectors, "frame", split_axis=1, concat_axis=0, tiled=True
    )
    asking_token_vectors, key_matrix_rows, value_matrix_rows = project_through(
        position_rows,
        asking_projection_tensor,
        lookup_projection_tensor,
        content_projection_tensor,
        logit_sharpness,
    )
    result = band_attention(asking_token_vectors, key_matrix_rows, value_matrix_rows)
    attended = lax.all_to_all(result, "frame", split_axis=0, concat_axis=1, tiled=True)
    flat_attended = attended.reshape(frames_dev * seq_len, -1)
    summed = jnp.dot(
        flat_attended, final_projection_tensor, preferred_element_type=jnp.float32
    ) + floated.reshape(frames_dev * seq_len, width)
    return summed.astype(jnp.bfloat16).reshape(frames_dev, seq_len, width)


MESH = pl.DeviceIdType.MESH
HIGH = HEADS_WIN * CHANNELS_PER_ATT


def fused(
    devices,
    local_frames,
    sharp_hbm,
    x_hbm,
    gain_hbm,
    wq_hbm,
    wk_hbm,
    wv_hbm,
    wo_hbm,
    done_ref,
    left_ref,
    x_own,
    wo,
    sharp_ref,
    gain_ref,
    wq,
    wk,
    wv,
    gathered,
    extra,
    q_rows,
    k_rows,
    v_rows,
    outgoing,
    outgoing_extra,
    returned,
    load_sem,
    ready,
    send_a,
    send_x,
    recv_a,
    recv_x,
    send_b,
    send_c,
    recv_b,
):
    me = lax.axis_index("frame")
    block, width = x_own.shape[1], x_own.shape[2]
    positions = block // local_frames
    chips = devices // 2
    depth = chips // 4
    half = devices // 2
    rows = half * block
    chip, side = me // 2, lax.rem(me, 2)
    partner = me + 1 - 2 * side
    z, y, x = chip // 4, lax.rem(chip // 2, 2), lax.rem(chip, 2)
    low = me < half

    def other(dz, dy, dx):
        tz = lax.rem(z + dz, depth)
        ty = y + dy - 2 * dy * y
        tx = x + dx - 2 * dx * x
        above = (tz >= z) & (ty >= y) & (tx >= x)
        below = (tz <= z) & (ty <= y) & (tx <= x)
        return tz * 4 + ty * 2 + tx, above, below

    steps = [(dz, dy, dx) for dz in range(depth) for dy in range(2) for dx in range(2)][1:]
    far_first = sorted(steps, key=lambda s: (s[0] == 0, s[0]))
    near_first = sorted(steps, key=lambda s: (sum(s), s[0]))

    x_load = pltpu.make_async_copy(x_hbm, x_own, load_sem.at[0])
    x_load.start()
    barrier = pltpu.get_barrier_semaphore()

    def signal(semaphore, target):
        pl.semaphore_signal(
            semaphore, inc=1, device_id={"frame": target}, device_id_type=MESH
        )

    signal(barrier, partner)
    for step in near_first:
        there, above, _ = other(*step)

        @pl.when(above)
        def _():
            signal(barrier, there * 2)
            signal(barrier, there * 2 + 1)

    loads = [
        pltpu.make_async_copy(source, target, load_sem.at[i + 1])
        for i, (source, target) in enumerate(
            (
                (sharp_hbm, sharp_ref),
                (gain_hbm, gain_ref),
                (wq_hbm, wq),
                (wk_hbm, wk),
                (wv_hbm, wv),
                (wo_hbm, wo),
            )
        )
    ]
    for load in loads:
        load.start()
    with jax.named_scope("barrier"):
        pl.semaphore_wait(barrier, 2 * ((z + 1) * (y + 1) * (x + 1) - 1) + 1)
    for step in far_first:
        there, _, below = other(*step)

        @pl.when(below)
        def _():
            signal(ready.at[chip], there * 2)
            signal(ready.at[chip], there * 2 + 1)

    with jax.named_scope("load_x"):
        x_load.wait()

    def remote(source, target, send, recv, device):
        pltpu.make_async_remote_copy(
            src_ref=source,
            dst_ref=target,
            send_sem=send,
            recv_sem=recv,
            device_id={"frame": device},
            device_id_type=MESH,
        ).start()

    layer = devices // depth
    layer_rows = layer * block

    def send_tokens(target):
        remote(x_own.at[target], gathered.at[me], send_a, recv_a.at[z], target)

    def send_extra(target):
        remote(x_own.at[target + 1 + half], extra.at[me], send_x, recv_x, target)

    shelf = depth // 2
    inner = z < shelf - 1

    def send_four(there):
        for s in range(2):
            send_tokens(there * 2 + s)
        send_extra(there * 2)

    with jax.named_scope("send_first"):
        send_tokens(partner)

        @pl.when(low & (side == 1))
        def _():
            send_extra(partner)

        @pl.when(low & (side == 0))
        def _():
            extra[me] = x_own[me + 1 + half]

        gathered[me] = x_own[me]

    def plane(step):
        return lax.rem(z + step[0], depth)

    def each_below(act):
        for step in far_first:
            there, _, below = other(*step)
            pl.when(below)(functools.partial(act, there))

    def each_joined(wanted, act):
        for step in near_first:
            dz, dy, dx = step
            there, above, _ = other(*step)

            @pl.when(above & wanted(step))
            def _():
                pl.semaphore_wait(ready.at[there], 2)
                act(there, step)
                ty, tx = lax.rem(there // 2, 2), lax.rem(there, 2)
                for p in range(depth) if dz == 0 else (None,):
                    tz = there // 4 if p is None else p
                    for ey in range(2 - dy):
                        for ex in range(2 - dx):
                            found = (y >= ey) & (x >= ex)
                            if p is not None:
                                found &= (p < z) | ((p == z) & (ey + ex > 0))
                            elif ey + ex == 0:
                                continue
                            pl.when(found)(
                                functools.partial(
                                    act, tz * 4 + (ty - ey) * 2 + tx - ex, step
                                )
                            )

    @pl.when(inner)
    def _():
        with jax.named_scope("send_group"):
            each_below(send_four)
            each_joined(lambda step: plane(step) < shelf, lambda there, step: send_four(there))

        with jax.named_scope("send_across"):
            each_joined(
                lambda step: plane(step) >= shelf, lambda there, step: send_tokens(there * 2)
            )
            for step in near_first:
                there, _, _ = other(*step)

                @pl.when(plane(step) >= shelf)
                def _():
                    send_tokens(there * 2 + 1)

    @pl.when(jnp.logical_not(inner))
    def _():
        with jax.named_scope("send_below"):
            each_below(lambda there: send_tokens(there * 2))

        with jax.named_scope("send_above"):
            each_joined(lambda step: True, lambda there, step: send_tokens(there * 2))

        with jax.named_scope("send_rest"):

            @pl.when(low)
            def _():
                for k in range(1, half // 2):
                    there = lax.rem(chip + k, half // 2)
                    send_tokens(there * 2 + 1)
                    send_extra(there * 2)

            for i in range(depth):
                upward = jnp.where(z == depth - 1, (i + shelf) % depth, i)
                tz = jnp.where(low, (i + shelf) % depth, upward)
                for dy in range(2):
                    for dx in range(2):
                        there, _, _ = other(lax.rem(tz - z + depth, depth), dy, dx)

                        @pl.when((there != chip) & (jnp.logical_not(low) | (tz >= shelf)))
                        def _():
                            send_tokens(there * 2 + 1)

    with jax.named_scope("load_rest"):
        for load in loads:
            load.wait()

    def arrived(ref, semaphore):
        pltpu.make_async_remote_copy(
            src_ref=ref,
            dst_ref=ref,
            send_sem=send_a,
            recv_sem=semaphore,
            device_id={"frame": partner},
            device_id_type=MESH,
        ).wait_recv()

    def departed(ref, semaphore):
        pltpu.make_async_remote_copy(
            src_ref=ref,
            dst_ref=ref,
            send_sem=semaphore,
            recv_sem=recv_x,
            device_id={"frame": partner},
            device_id_type=MESH,
        ).wait_send()

    def project(tokens, place, ask=True):
        tokens = tokens.reshape(-1, width).astype(jnp.float32)
        normed = (quadratic_average_rescaling(tokens) * gain_ref[...].reshape(1, width)).astype(
            jnp.bfloat16
        )
        q = jnp.dot(normed, wq[...], preferred_element_type=jnp.float32) if ask else None
        k = jnp.dot(normed, wk[...], preferred_element_type=jnp.float32)
        v = jnp.dot(normed, wv[...], preferred_element_type=jnp.float32)
        b = slice(place, place + tokens.shape[0])
        for h in range(HEADS_WIN):
            c = slice(h * CHANNELS_PER_ATT, (h + 1) * CHANNELS_PER_ATT)
            if ask:
                q_rows[b, c] = (
                    quadratic_average_rescaling(q[:, c]) * sharp_ref[h] / math.sqrt(CHANNELS_PER_ATT)
                ).astype(jnp.bfloat16)
            k_rows[b, c] = quadratic_average_rescaling(k[:, c]).astype(jnp.bfloat16)
            v_rows[b, c] = v[:, c].astype(jnp.bfloat16)

    def ids(first, count, axis):
        shape = (count, 1) if axis == 0 else (1, count)
        r = first + lax.broadcasted_iota(jnp.int32, shape, axis)
        owner = r // block
        inner = r - owner * block
        return owner * local_frames + inner // positions, inner % positions

    def attend(asking, keys, target):
        first, count = asking
        start, length = keys
        base = 2 * rows if start >= 2 * rows else 0
        t_row, p_row = ids(first - base, count, 0)
        t_col, p_col = ids(start - base, length, 1)
        offset = t_row - t_col
        inside = (p_row == p_col) & (offset >= 0) & (offset < WINDOW)
        a, b = slice(first, first + count), slice(start, start + length)
        heads = [slice(h * CHANNELS_PER_ATT, (h + 1) * CHANNELS_PER_ATT) for h in range(HEADS_WIN)]
        scores = [
            lax.dot_general(
                q_rows[a, c],
                k_rows[b, c],
                (((1,), (1,)), ((), ())),
                preferred_element_type=jnp.float32,
            )
            for c in heads
        ]
        weights = [softmax_bf16(s, inside) for s in scores]
        attended = [
            jnp.dot(w, v_rows[b, c], preferred_element_type=jnp.float32)
            for w, c in zip(weights, heads)
        ]
        for c, part in zip(heads, attended):
            target[:, :, c] = part.reshape(count // block, block, CHANNELS_PER_ATT).astype(
                jnp.bfloat16
            )

    def send_back(target):
        remote(outgoing.at[target], returned.at[side, chip], send_b, recv_b.at[side], target)

    def back_to_layer(p):
        for k in range(layer // 2):
            there = p * (layer // 2) + lax.rem(chip + k, layer // 2)
            for s in range(2):
                target = there * 2 + s

                @pl.when(target != me)
                def _():
                    send_back(target)

    def wait_layer(p):
        @pl.when(z == p)
        def _():
            arrived(gathered.at[pl.ds(0, layer - 1)], recv_a.at[p])

        @pl.when(z != p)
        def _():
            arrived(gathered.at[pl.ds(0, layer)], recv_a.at[p])

    lower, upper = range(shelf), range(shelf, depth)

    @pl.when(low)
    def _():
        with jax.named_scope("wait_own"):
            for p in lower:
                wait_layer(p)
        with jax.named_scope("work_own"):
            project(gathered[:half], 0)
            attend((0, rows), (0, rows), outgoing.at[pl.ds(0, half)])
            for k in range(1, half):
                send_back(lax.rem(me + k, half))
            returned[side, chip] = outgoing[me]

        for p in reversed(upper):
            with jax.named_scope(f"wait_far{p}"):
                wait_layer(p)
            with jax.named_scope(f"work_far{p}"):
                project(gathered[p * layer : (p + 1) * layer], p * layer_rows)
        with jax.named_scope("work_back"):
            attend((rows, rows), (0, 2 * rows), outgoing.at[pl.ds(half, half)])
            for k in range(layer // 2):
                for p in upper:
                    there = p * (layer // 2) + lax.rem(chip + k, layer // 2)
                    send_back(there * 2)
                    send_back(there * 2 + 1)

        @pl.when(side == 0)
        def _():
            with jax.named_scope("wait_extra"):
                arrived(extra.at[pl.ds(0, half - 1)], recv_x)
            with jax.named_scope("work_extra"):
                project(extra[...], 2 * rows)
                attend((2 * rows, rows), (2 * rows, rows), outgoing_extra)
                for k in range(1, half):
                    target = lax.rem(me + k, half)
                    remote(
                        outgoing_extra.at[target],
                        returned.at[1, chip + half // 2],
                        send_c,
                        recv_b.at[1],
                        target,
                    )
                returned[1, chip + half // 2] = outgoing_extra[me]

    @pl.when(jnp.logical_not(low))
    def _():
        with jax.named_scope("wait_own"):
            for p in upper:
                wait_layer(p)
        with jax.named_scope("work_own"):
            project(gathered[half:], rows)
        with jax.named_scope("wait_far"):
            for p in lower:
                wait_layer(p)

        @pl.when(side == 0)
        def _():
            with jax.named_scope("work_far"):
                project(gathered[:half], 0)
                attend((0, rows), (0, rows), outgoing.at[pl.ds(0, half)])
                for k in range(half):
                    send_back(lax.rem(me + k, half))
                attend((rows, rows), (0, 2 * rows), outgoing.at[pl.ds(half, half)])
                for p in upper:
                    back_to_layer(p)

        @pl.when(side == 1)
        def _():
            with jax.named_scope("work_far"):
                project(gathered[:half], 0, ask=False)
                attend((rows, rows), (0, 2 * rows), outgoing.at[pl.ds(half, half)])
                for p in upper:
                    back_to_layer(p)

        returned[side, chip] = outgoing[me]

    for s in range(2):
        with jax.named_scope(f"wait_b{s}"):
            fewer = (side == s) | low if s else side == s

            @pl.when(fewer)
            def _():
                arrived(returned.at[s, pl.ds(0, half - 1)], recv_b.at[s])

            @pl.when(jnp.logical_not(fewer))
            def _():
                arrived(returned.at[s], recv_b.at[s])

        with jax.named_scope(f"finish{s}"):
            if s:
                left_ref[...] = returned[s].reshape(rows, HIGH)
            else:
                summed = jnp.dot(
                    returned[s].reshape(rows, HIGH), wo[...], preferred_element_type=jnp.float32
                )
                for k in range(half):
                    done_ref[k] = (
                        summed[k * block : (k + 1) * block] + x_own[2 * k].astype(jnp.float32)
                    ).astype(jnp.bfloat16)

    with jax.named_scope("departed"):
        departed(x_own.at[pl.ds(0, devices - 1)], send_a)

        @pl.when(low & (side == 0))
        def _():
            departed(x_own.at[pl.ds(0, half // 2 - 1)], send_x)
            departed(outgoing_extra.at[pl.ds(0, half - 1)], send_c)

        @pl.when(low & (side == 1))
        def _():
            departed(x_own.at[pl.ds(0, half // 2)], send_x)

        @pl.when(low | (side == 0))
        def _():
            departed(outgoing.at[pl.ds(0, devices - 1)], send_b)

        @pl.when(jnp.logical_not(low) & (side == 1))
        def _():
            departed(outgoing.at[pl.ds(0, half - 1)], send_b)


def finish(done, left, x_own, wo, result, held, sem):
    half, block, width = done.shape
    first = pltpu.make_async_copy(done, result.at[:, 0], sem.at[0])
    first.start()
    pieces = sem.shape[0] - 1
    share = width // pieces
    copies = []
    for n in range(pieces):
        c = slice(n * share, (n + 1) * share)
        summed = jnp.dot(left[...], wo[:, c], preferred_element_type=jnp.float32)
        for k in range(half):
            held[k, :, c] = (
                summed[k * block : (k + 1) * block] + x_own[2 * k + 1, :, c].astype(jnp.float32)
            ).astype(jnp.bfloat16)
        copies.append(
            pltpu.make_async_copy(
                held.at[:, :, pl.ds(n * share, share)],
                result.at[:, 1, :, pl.ds(n * share, share)],
                sem.at[n + 1],
            )
        )
        copies[-1].start()
    first.wait()
    for copy in copies:
        copy.wait()


def local_fused(devices, x, gain, wq, wk, wv, sharp, wo):
    local_frames, seq_len, width = x.shape
    positions = seq_len // devices
    block = local_frames * positions
    half = devices // 2
    rows = half * block
    blocks = x.reshape(local_frames, devices, positions, width)
    blocks = blocks.transpose(1, 0, 2, 3).reshape(devices, block, width)
    vmem = pl.BlockSpec(memory_space=pltpu.VMEM)
    anywhere = pl.BlockSpec(memory_space=pl.ANY)
    dma = pltpu.SemaphoreType.DMA
    held = (half, block, width)
    parts = pl.pallas_call(
        functools.partial(fused, devices, local_frames),
        out_shape=[
            pltpu.VMEM(held, jnp.bfloat16),
            pltpu.VMEM((rows, HIGH), jnp.bfloat16),
            pltpu.VMEM(blocks.shape, jnp.bfloat16),
            pltpu.VMEM(wo.shape, jnp.bfloat16),
        ],
        in_specs=[anywhere] * 7,
        out_specs=[vmem] * 4,
        scratch_shapes=[
            pltpu.SMEM(sharp.shape, jnp.float32),
            pltpu.VMEM(gain.shape, jnp.float32),
            pltpu.VMEM(wq.shape, jnp.bfloat16),
            pltpu.VMEM(wk.shape, jnp.bfloat16),
            pltpu.VMEM(wv.shape, jnp.bfloat16),
            pltpu.VMEM(blocks.shape, jnp.bfloat16),
            pltpu.VMEM((half, block, width), jnp.bfloat16),
            pltpu.VMEM((3 * rows, HIGH), jnp.bfloat16),
            pltpu.VMEM((3 * rows, HIGH), jnp.bfloat16),
            pltpu.VMEM((3 * rows, HIGH), jnp.bfloat16),
            pltpu.VMEM((devices, block, HIGH), jnp.bfloat16),
            pltpu.VMEM((half, block, HIGH), jnp.bfloat16),
            pltpu.VMEM((2, half, block, HIGH), jnp.bfloat16),
            dma((7,)),
            pltpu.SemaphoreType.REGULAR((devices // 2,)),
            dma,
            dma,
            dma((devices // 8,)),
            dma,
            dma,
            dma,
            dma((2,)),
        ],
        compiler_params=pltpu.CompilerParams(
            collective_id=0, has_side_effects=True, vmem_limit_bytes=60 * 2**20
        ),
    )(sharp, blocks, gain, wq, wk, wv, wo)
    out = pl.pallas_call(
        finish,
        out_shape=jax.ShapeDtypeStruct((half, 2, block, width), jnp.bfloat16),
        in_specs=[vmem] * 4,
        out_specs=anywhere,
        scratch_shapes=[pltpu.VMEM(held, jnp.bfloat16), dma((3,))],
    )(*[pltpu.with_memory_space_constraint(part, pltpu.VMEM) for part in parts])
    out = out.reshape(devices, local_frames, positions, width).transpose(1, 0, 2, 3)
    return out.reshape(x.shape)


def solution(mesh):
    devices = mesh.shape["frame"]

    def body(x, *rest):
        positions = x.shape[1] // devices
        if devices % 16 == 0 and positions % 8 == 0:
            return local_fused(devices, x, *rest)
        return local(x, *rest)

    placed = (P(("clips", "frame"), None, None), P(), P(), P(), P(), P(), P())
    return jax.shard_map(
        body,
        mesh=mesh,
        in_specs=placed,
        out_specs=P(("clips", "frame"), None, None),
        check_vma=False,
    )
```
